32 devices in a mesh: inst: 4 (over x, core), gx: 2 (over y), gy: 4 (over z).
Axes of the slice: x: 2, y: 2, z: 4, core: 2. Of those that a mesh axis runs over, the one named last changes fastest.
Arguments:
- state: float32 [8, 5, 16, 32, 128], P('inst', None, 'gx', 'gy'), may hold values from -6 to 6
- source: float32 [8, 5, 16, 32, 128], P('inst', None, 'gx', 'gy'), may hold values from -60 to 60
- jacobian: float32 [8, 5, 5, 16, 32, 128], P('inst', None, None, 'gx', 'gy'), may hold values from -1.5 to 16, as said below
- couplings: float32 [6, 5, 5], replicated, may hold values from -0.625 to 0.625
- omega: float32 [1], replicated, may hold values from 0.2 to 0.6
Outputs:
- state_next: float32 [8, 5, 16, 32, 128], P('inst', None, 'gx', 'gy')
- last_residual: float32 [8, 5, 16, 32, 128], P('inst', None, 'gx', 'gy')
The draws below stay inside these ranges and needn't reach their ends.
Inputs may be any that keep to these rules, and one draw needn't show every extreme that they name: In every block jacobian[n, :, :, cell] each diagonal entry lies in 8 to 16 and exceeds the sum of magnitudes of the other entries of its row by 2 or more.
All inputs are finite; a program needn't handle non-finite values.
Results may differ from the reference program's by a relative error of at most 0.0003.
Values sent between devices are 32-bit elements; how exact they have to be, the bound alone decides.
A program may use at most 64 MiB of HBM per device.

```python
import math
import jax
import jax.numpy as jnp
from jax import lax

NVAR = 5
NT = 8
ITERS = 3
NX = 16
NY = 32
NZ = 128


def draw_jacobian(key, part):
    first_key, second_key = jax.random.split(jax.random.fold_in(key, 17))
    shape = (NT, NVAR, NVAR, NX, NY, NZ)
    diagonal = jax.random.uniform(first_key, (NT, NVAR, NX, NY, NZ), jnp.float32, 8.0, 16.0)
    others = jnp.clip(0.6 * jax.random.normal(second_key, shape, jnp.float32), -1.5, 1.5)
    identity = jnp.eye(NVAR, dtype=jnp.float32)[None, :, :, None, None, None]
    return others * (1.0 - identity) + identity * diagonal[:, :, None]


def shard_levels(stream_key, shape, shards, least, largest):
    level, own = 1.0, jax.random.fold_in(stream_key, 6)
    for axis_at, blocks in shards:
        heights = jnp.exp(jax.random.uniform(jax.random.fold_in(own, axis_at), (blocks,), jnp.float32, least / len(shards), largest / len(shards)))
        level = level * jnp.repeat(heights, shape[axis_at] // blocks).reshape([-1 if axis == axis_at else 1 for axis in range(len(shape))])
    return level


def bell_draw(key, shape, scale, most, cuts=(), held_as=jnp.bfloat16):
    drawn = scale * jax.random.normal(key, shape, jnp.float32)
    if cuts:
        drawn = drawn * shard_levels(key, shape, cuts, -0.22, 0.18)
    return jnp.clip(drawn, -most, most).astype(held_as)


def setup_inputs(seed: int = 0) -> dict:
    streams_of = jax.random.split(jax.random.key(seed), 6)
    return {
        "state": bell_draw(streams_of[0], (NT, NVAR, NX, NY, NZ), 1.0, 6.0, ((0, 4), (2, 2), (3, 4)), jnp.float32),
        "source": bell_draw(streams_of[1], (NT, NVAR, NX, NY, NZ), 10.0, 60.0, ((0, 4), (2, 2), (3, 4)), jnp.float32),
        "jacobian": draw_jacobian(jax.random.fold_in(streams_of[5], 71), 0),
        "couplings": bell_draw(streams_of[3], (6, NVAR, NVAR), 100 ** -0.5, 0.625, (), jnp.float32),
        "omega": jnp.clip(jnp.exp(jax.random.uniform(streams_of[4], (1,), jnp.float32, math.log(0.2), math.log(0.6))), 0.2, 0.6),
    }


def spectral_table(row_index, column_index, total):
    offset = (row_index[:, None] - column_index[None, :]).astype(jnp.int32)
    parity = 1.0 - 2.0 * jnp.mod(offset, 2).astype(jnp.float32)
    angle = jnp.pi * offset.astype(jnp.float32) / total
    onsite = offset == 0
    sine = jnp.where(onsite, jnp.ones_like(angle), jnp.sin(angle))
    return jnp.where(onsite, jnp.zeros_like(angle), 0.5 * parity * jnp.cos(angle) / sine)


def pad_field(field):
    wrapped = jnp.concatenate([field[:, :, -1:], field, field[:, :, :1]], axis=2)
    return jnp.pad(wrapped, ((0, 0), (1, 1), (0, 0), (1, 1)))


def neighbours(padded, couplings):
    shifted = [padded[:, :-2, 1:-1, 1:-1], padded[:, 2:, 1:-1, 1:-1],
               padded[:, 1:-1, :-2, 1:-1], padded[:, 1:-1, 2:, 1:-1],
               padded[:, 1:-1, 1:-1, :-2], padded[:, 1:-1, 1:-1, 2:]]
    result = jnp.zeros(shifted[0].shape, jnp.float32)
    for direction in range(6):
        result = result + jnp.einsum("vw,wxyz->vxyz", couplings[direction], shifted[direction],
                                     precision=lax.Precision.HIGHEST)
    return result


def solve_blocks(blocks, right):
    size = blocks.shape[0]
    matrix = [[blocks[row, column] for column in range(size)] for row in range(size)]
    vector = [right[row] for row in range(size)]
    for pivot in range(size):
        for target in range(pivot + 1, size):
            factor = matrix[target][pivot] / matrix[pivot][pivot]
            for column in range(pivot + 1, size):
                matrix[target][column] = matrix[target][column] - factor * matrix[pivot][column]
            vector[target] = vector[target] - factor * vector[pivot]
    result = [None] * size
    for pivot in reversed(range(size)):
        total = vector[pivot]
        for column in range(pivot + 1, size):
            total = total - matrix[pivot][column] * result[column]
        result[pivot] = total / matrix[pivot][pivot]
    return jnp.stack(result, axis=0)


def reference(state, source, jacobian, couplings, omega):
    total = state.shape[0]
    positions = jnp.arange(total, dtype=jnp.int32)
    table = spectral_table(positions, positions, total)
    current = state
    residual = state
    for repeat in range(ITERS):
        spectral = omega[0] * jnp.einsum("nm,mvxyz->nvxyz", table, current,
                                         precision=lax.Precision.HIGHEST)

        def one_instance(pieces):
            field, blocks, right_side, spec_part = pieces
            beside = neighbours(pad_field(field), couplings)
            diagonal_part = jnp.einsum("vwxyz,wxyz->vxyz", blocks, field,
                                       precision=lax.Precision.HIGHEST)
            resid = right_side - diagonal_part - beside - spec_part
            return field + solve_blocks(blocks, resid), resid

        current, residual = lax.map(one_instance, (current, jacobian, source, spectral))
    return current, residual
```

```python
import functools
import math

import jax
import jax.numpy as jnp
from jax import lax
from jax.experimental import pallas as pl
from jax.experimental.pallas import tpu as pltpu
from jax.sharding import PartitionSpec as P

ITERS = 3
LAG = 2
MESH = pl.DeviceIdType.MESH


def derivative(offset, total):
    offset = offset % total
    if offset > total // 2:
        offset -= total
    if offset == 0:
        return 0.0
    angle = math.pi * offset / total
    return 0.5 * (-1.0) ** offset * math.cos(angle) / math.sin(angle)


def factor(blocks):
    size = len(blocks)
    matrix = [list(row) for row in blocks]
    for pivot in range(size):
        matrix[pivot][pivot] = 1.0 / matrix[pivot][pivot]
        for target in range(pivot + 1, size):
            ratio = matrix[target][pivot] * matrix[pivot][pivot]
            matrix[target][pivot] = ratio
            for column in range(pivot + 1, size):
                matrix[target][column] = matrix[target][column] - ratio * matrix[pivot][column]
    return matrix


def substitute(matrix, right):
    size = len(right)
    vector = list(right)
    for pivot in range(size):
        for target in range(pivot + 1, size):
            vector[target] = vector[target] - matrix(target, pivot) * vector[pivot]
    result = [None] * size
    for pivot in reversed(range(size)):
        total = vector[pivot]
        for column in range(pivot + 1, size):
            total = total - matrix(pivot, column) * result[column]
        result[pivot] = total * matrix(pivot, pivot)
    return result


def weighted(weights, pieces):
    total = None
    for weight, piece in zip(weights, pieces):
        if isinstance(weight, float) and weight == 0.0:
            continue
        term = weight * piece
        total = term if total is None else total + term
    return total


def kernel(
    ranks, count_x, count_y,
    state, source, jacobian, couplings, omega,
    state_next, last_residual,
    cur, peer, part, got, relayed, edge_out, edge_in,
    rhs, blocks, lu, weights_in, speed_in,
    load_sem, x_send, core_send, edge_send, side_send,
    first_recv, peer_recv, relay_recv, got_recv, edge_recv, side_recv,
):
    local, nvar, planes, rows, depth = state.shape
    total = local * ranks
    pairs = ranks // 2
    rank = lax.axis_index("inst")
    at_x = lax.axis_index("gx")
    at_y = lax.axis_index("gy")
    pair = rank // 2
    core = rank % 2
    partner = pair * 2 + 1 - core
    up = (at_y + 1) % count_y
    down = (at_y + count_y - 1) % count_y
    has_low = at_x > 0
    has_high = at_x < count_x - 1
    flip = at_x % 2 == 0
    hops = range(1, pairs)

    def plane_of(step):
        return jnp.where(flip, planes - 1 - step, step)

    def load_state(x):
        return pltpu.make_async_copy(state.at[:, :, x], cur.at[0, x + 1], load_sem.at[0])

    loads = [
        pltpu.make_async_copy(jacobian, blocks, load_sem.at[1]),
        pltpu.make_async_copy(source, rhs, load_sem.at[2]),
        pltpu.make_async_copy(couplings, weights_in, load_sem.at[3]),
        pltpu.make_async_copy(omega, speed_in, load_sem.at[4]),
    ]

    def remote(source_ref, target_ref, send, recv, **where):
        return pltpu.make_async_remote_copy(
            source_ref, target_ref, send, recv, device_id=where, device_id_type=MESH)

    def to_peer(k, x):
        recv = first_recv.at[0] if k == 0 else peer_recv.at[k - 1, x]
        return remote(cur.at[k, x + 1], peer.at[k, x], core_send.at[0], recv, inst=partner)

    def to_pair(k, x, hop):
        target = ((pair + hop) % pairs) * 2 + core
        outgoing = cur.at[0, x + 1] if k == 0 else part.at[k - 1, hop - 1, x]
        return remote(
            outgoing, got.at[k, hop - 1, x], x_send.at[0], got_recv.at[k % 2, hop - 1, x],
            inst=target)

    def relay(x, hop):
        return remote(
            got.at[0, hop - 1, x], relayed.at[hop - 1, x], core_send.at[1],
            relay_recv.at[hop - 1, x], inst=partner)

    def to_side(k, x, side):
        return remote(
            edge_out.at[k, x, side], edge_in.at[k, x, side], edge_send.at[0],
            edge_recv.at[k % 2, x], gy=up if side == 0 else down)

    def both_sides(k, x):
        return remote(
            edge_out.at[k, x], edge_in.at[k, x], edge_send.at[0], edge_recv.at[k % 2, x], gy=up)

    def to_next(k):
        return remote(
            cur.at[k, planes], cur.at[k, 0], side_send.at[0], side_recv.at[0, k], gx=at_x + 1)

    def to_last(k):
        return remote(
            cur.at[k, 1], cur.at[k, planes + 1], side_send.at[1], side_recv.at[1, k],
            gx=at_x - 1)

    def send_planes(k, x):
        to_peer(k, x).start()

        @pl.when(jnp.logical_and(x == planes - 1, has_high))
        def _():
            to_next(k).start()

        @pl.when(jnp.logical_and(x == 0, has_low))
        def _():
            to_last(k).start()

    def send_edges(k, x, field):
        for n in range(local):
            for v in range(nvar):
                at = n * nvar + v
                edge_out[k, x, 1, at:at + 1] = field[n][v][:1]
                edge_out[k, x, 0, at:at + 1] = field[n][v][rows - 1:]

    def start_edges(k, x):
        to_side(k, x, 0).start()
        to_side(k, x, 1).start()

    def mine(k, x):
        return [[cur[k, x + 1, n, v] for v in range(nvar)] for n in range(local)]

    even = core == 0

    def weights_of(hop, a):
        own = [derivative(2 * local * hop + a - b, total) for b in range(local)]
        other = [
            jnp.where(
                even,
                jnp.float32(derivative(2 * local * hop - local + a - b, total)),
                jnp.float32(derivative(2 * local * hop + local + a - b, total)),
            )
            for b in range(local)
        ]
        return own + other

    def send_parts(k, x):
        to_peer(k, x).wait_recv()
        for hop in hops:
            for a in range(local):
                weights = weights_of(hop, a)
                for v in range(nvar):
                    pieces = [cur[k, x + 1, b, v] for b in range(local)]
                    pieces += [peer[k, x, b, v] for b in range(local)]
                    part[k - 1, hop - 1, x, a, v] = weighted(weights, pieces)
            to_pair(k, x, hop).start()

    for step in range(planes):
        load_state(plane_of(step)).start()
    for copy in loads:
        copy.start()

    barrier = pltpu.get_barrier_semaphore()

    def greet(**where):
        pl.semaphore_signal(barrier, inc=1, device_id=where, device_id_type=MESH)

    greet(inst=partner)
    for hop in hops:
        greet(inst=((pair + hop) % pairs) * 2 + core)
    greet(gy=up)
    greet(gy=down)

    @pl.when(has_low)
    def _():
        greet(gx=at_x - 1)

    @pl.when(has_high)
    def _():
        greet(gx=at_x + 1)

    zero = jnp.zeros((local, nvar, rows, depth), jnp.float32)

    @pl.when(jnp.logical_not(has_low))
    def _():
        for k in range(ITERS):
            cur[k, 0] = zero

    @pl.when(jnp.logical_not(has_high))
    def _():
        for k in range(ITERS):
            cur[k, planes + 1] = zero

    sides = has_low.astype(jnp.int32) + has_high.astype(jnp.int32)
    held = cur.at[0, 1:planes + 1]
    pltpu.make_async_copy(held, held, load_sem.at[0]).wait()
    pl.semaphore_wait(barrier, pairs + 2 + sides)

    @pl.loop(0, planes)
    def _(step):
        x = plane_of(step)
        for hop in hops:
            to_pair(0, x, hop).start()

    @pl.loop(0, planes)
    def _(step):
        x = plane_of(step)
        send_edges(0, x, mine(0, x))
        send_planes(0, x)
        start_edges(0, x)

    for copy in loads:
        copy.wait()

    @pl.loop(0, planes)
    def _(step):
        x = plane_of(step)
        for n in range(local):
            matrix = factor([[blocks[n, v, w, x] for w in range(nvar)] for v in range(nvar)])
            for v in range(nvar):
                for w in range(nvar):
                    lu[n, v, w, x] = matrix[v][w]

    row_at = lax.broadcasted_iota(jnp.int32, (rows, depth), 0)
    lane_at = lax.broadcasted_iota(jnp.int32, (rows, depth), 1)
    first_row, final_row = row_at == 0, row_at == rows - 1
    first_lane, final_lane = lane_at == 0, lane_at == depth - 1
    speed = speed_in[0]
    lag = min(LAG, planes)

    def near_side(k, x):
        result = [[None] * nvar for _ in range(local)]
        for w in range(nvar):
            for n in range(local):
                field = cur[k, x + 1, n, w]
                at = n * nvar + w
                shifted = [
                    cur[k, x, n, w],
                    cur[k, x + 2, n, w],
                    jnp.where(first_row, edge_in[k, x, 0, at:at + 1], pltpu.roll(field, 1, 0)),
                    jnp.where(
                        final_row, edge_in[k, x, 1, at:at + 1], pltpu.roll(field, rows - 1, 0)),
                    jnp.where(first_lane, 0.0, pltpu.roll(field, 1, 1)),
                    jnp.where(final_lane, 0.0, pltpu.roll(field, depth - 1, 1)),
                ]
                for v in range(nvar):
                    term = weighted([weights_in[v, d, w] for d in range(6)], shifted)
                    last = result[n][v]
                    result[n][v] = term if last is None else last + term
        for n in range(local):
            weights = weights_of(0, n)
            for v in range(nvar):
                pieces = [cur[k, x + 1, b, v] for b in range(local)]
                pieces += [peer[k, x, b, v] for b in range(local)]
                spectral = weighted(weights, pieces)
                result[n][v] = rhs[n, v, x] - result[n][v] - speed * spectral
        return result

    def far_side(k, x, n, v):
        spectral = None
        for hop in hops:
            if k == 0:
                pieces = [got[k, hop - 1, x, b, v] for b in range(local)]
                pieces += [relayed[hop - 1, x, b, v] for b in range(local)]
                term = weighted(weights_of(hop, n), pieces)
            else:
                term = got[k, hop - 1, x, n, v]
            spectral = term if spectral is None else spectral + term
        return spectral

    def pass_on(x):
        for hop in hops:
            to_pair(0, x, hop).wait_recv()
            relay(x, hop).start()

    pass_on(plane_of(0))
    pltpu.make_async_copy(peer.at[0], peer.at[0], first_recv.at[0]).wait()

    for k in range(ITERS):
        final_pass = k == ITERS - 1

        @pl.loop(0, planes)
        def _(step, k=k, final_pass=final_pass):
            x = plane_of(step)

            @pl.when(jnp.logical_and(x == 0, has_low))
            def _():
                to_next(k).wait_recv()

            @pl.when(jnp.logical_and(x == planes - 1, has_high))
            def _():
                to_last(k).wait_recv()

            both_sides(k, x).wait_recv()
            rights = near_side(k, x)
            if final_pass:
                own = mine(k, x)
                for n in range(local):
                    for v in range(nvar):
                        for w in range(nvar):
                            rights[n][v] = rights[n][v] - blocks[n, v, w, x] * own[n][w]
            if k == 0:

                @pl.when(step + 1 < planes)
                def _():
                    pass_on(plane_of(step + 1))

                for hop in hops:
                    relay(x, hop).wait_recv()
            else:
                for hop in hops:
                    to_pair(k, x, hop).wait_recv()
            fields = []
            for n in range(local):
                right = rights[n]
                if pairs > 1:
                    right = [right[v] - speed * far_side(k, x, n, v) for v in range(nvar)]
                answer = substitute(lambda v, w: lu[n, v, w, x], right)
                for v in range(nvar):
                    if final_pass:
                        last_residual[n, v, x] = right[v]
                        state_next[n, v, x] = own[n][v] + answer[v]
                    else:
                        cur[k + 1, x + 1, n, v] = answer[v]
                fields.append(answer)
            if not final_pass:
                send_edges(k + 1, x, fields)
                send_planes(k + 1, x)
                start_edges(k + 1, x)

                @pl.when(step >= lag)
                def _():
                    send_parts(k + 1, plane_of(step - lag))

            if k > 0:

                @pl.when(step < lag)
                def _():
                    send_parts(k, plane_of(planes - lag + step))

    for hop in hops:
        sent = got.at[:, hop - 1]
        remote(sent, sent, x_send.at[0], x_send.at[0], inst=partner).wait_send()
    remote(peer, peer, core_send.at[0], core_send.at[0], inst=partner).wait_send()
    remote(relayed, relayed, core_send.at[1], core_send.at[1], inst=partner).wait_send()
    remote(edge_out, edge_out, edge_send.at[0], edge_send.at[0], inst=partner).wait_send()
    layer = cur.at[:, 0]

    @pl.when(has_high)
    def _():
        remote(layer, layer, side_send.at[0], side_send.at[0], inst=partner).wait_send()

    @pl.when(has_low)
    def _():
        remote(layer, layer, side_send.at[1], side_send.at[1], inst=partner).wait_send()


def store(field, residual, state_next, last_residual, sems):
    copies = [
        pltpu.make_async_copy(field, state_next, sems.at[0]),
        pltpu.make_async_copy(residual, last_residual, sems.at[1]),
    ]
    for copy in copies:
        copy.start()
    for copy in copies:
        copy.wait()


def solution(mesh):
    ranks, count_x, count_y = mesh.shape["inst"], mesh.shape["gx"], mesh.shape["gy"]

    def shards(state, source, jacobian, couplings, omega):
        local, nvar, planes, rows, depth = state.shape
        pairs = ranks // 2
        cell = (local, nvar, rows, depth)
        edge = pltpu.VMEM((ITERS, planes, 2, local * nvar, depth), jnp.float32)
        hbm = pl.BlockSpec(memory_space=pltpu.HBM)
        near = pl.BlockSpec(memory_space=pltpu.VMEM)
        dma = pltpu.SemaphoreType.DMA
        vmem = lambda *lead: pltpu.VMEM(lead + cell, jnp.float32)
        matrices = pltpu.VMEM(jacobian.shape, jnp.float32)
        flows = couplings.transpose(1, 0, 2)
        field, residual = pl.pallas_call(
            functools.partial(kernel, ranks, count_x, count_y),
            out_shape=[pltpu.VMEM(state.shape, jnp.float32)] * 2,
            in_specs=[hbm] * 5,
            out_specs=[near, near],
            scratch_shapes=[
                vmem(ITERS, planes + 2), vmem(ITERS, planes),
                vmem(ITERS - 1, pairs - 1, planes), vmem(ITERS, pairs - 1, planes),
                vmem(pairs - 1, planes), edge, edge,
                pltpu.VMEM(state.shape, jnp.float32), matrices, matrices,
                pltpu.SMEM(flows.shape, jnp.float32), pltpu.SMEM(omega.shape, jnp.float32),
                dma((5,)), dma((1,)), dma((2,)), dma((1,)), dma((2,)),
                dma((1,)), dma((ITERS - 1, planes)), dma((pairs - 1, planes)),
                dma((2, pairs - 1, planes)), dma((2, planes)), dma((2, ITERS)),
            ],
            compiler_params=pltpu.CompilerParams(
                collective_id=0, has_side_effects=True, vmem_limit_bytes=60 * 1024 * 1024),
            name="smooth",
        )(state, source, jacobian, flows, omega)
        return tuple(pl.pallas_call(
            store,
            out_shape=[jax.ShapeDtypeStruct(state.shape, jnp.float32)] * 2,
            in_specs=[near, near],
            out_specs=[hbm, hbm],
            scratch_shapes=[dma((2,))],
            compiler_params=pltpu.CompilerParams(vmem_limit_bytes=16 * 1024 * 1024),
            name="store",
        )(field, residual))

    split = P("inst", None, "gx", "gy", None)
    return jax.shard_map(
        shards,
        mesh=mesh,
        in_specs=(split, split, P("inst", None, None, "gx", "gy", None), P(), P()),
        out_specs=(split, split),
        check_vma=False,
    )
```

```python
import functools
import math

import jax
import jax.numpy as jnp
from jax import lax
from jax.experimental import pallas as pl
from jax.experimental.pallas import tpu as pltpu
from jax.sharding import PartitionSpec as P

ITERS = 3
LAG = 2
MESH = pl.DeviceIdType.MESH


def derivative(offset, total):
    offset = offset % total
    if offset > total // 2:
        offset -= total
    if offset == 0:
        return 0.0
    angle = math.pi * offset / total
    return 0.5 * (-1.0) ** offset * math.cos(angle) / math.sin(angle)


def factor(blocks):
    size = len(blocks)
    matrix = [list(row) for row in blocks]
    for pivot in range(size):
        matrix[pivot][pivot] = 1.0 / matrix[pivot][pivot]
        for target in range(pivot + 1, size):
            ratio = matrix[target][pivot] * matrix[pivot][pivot]
            matrix[target][pivot] = ratio
            for column in range(pivot + 1, size):
                matrix[target][column] = matrix[target][column] - ratio * matrix[pivot][column]
    return matrix


def substitute(matrix, right):
    size = len(right)
    vector = list(right)
    for pivot in range(size):
        for target in range(pivot + 1, size):
            vector[target] = vector[target] - matrix(target, pivot) * vector[pivot]
    result = [None] * size
    for pivot in reversed(range(size)):
        total = vector[pivot]
        for column in range(pivot + 1, size):
            total = total - matrix(pivot, column) * result[column]
        result[pivot] = total * matrix(pivot, pivot)
    return result


def weighted(weights, pieces):
    total = None
    for weight, piece in zip(weights, pieces):
        if isinstance(weight, float) and weight == 0.0:
            continue
        term = weight * piece
        total = term if total is None else total + term
    return total


def kernel(
    ranks, count_x, count_y,
    state, source, jacobian, couplings, omega,
    state_next, last_residual,
    cur, peer, part, got, relayed, edge_out, edge_in,
    rhs, blocks, lu, weights_in, speed_in,
    load_sem, x_send, core_send, edge_send, side_send,
    first_recv, peer_recv, relay_recv, got_recv, edge_recv, side_recv, ready,
):
    local, nvar, planes, rows, depth = state.shape
    total = local * ranks
    pairs = ranks // 2
    rank = lax.axis_index("inst")
    at_x = lax.axis_index("gx")
    at_y = lax.axis_index("gy")
    pair = rank // 2
    core = rank % 2
    partner = pair * 2 + 1 - core
    up = (at_y + 1) % count_y
    down = (at_y + count_y - 1) % count_y
    has_low = at_x > 0
    has_high = at_x < count_x - 1
    flip = at_x % 2 == 0
    hops = range(1, pairs)

    def plane_of(step):
        return jnp.where(flip, planes - 1 - step, step)

    def load_state(x):
        return pltpu.make_async_copy(state.at[:, :, x], cur.at[0, x + 1], load_sem.at[0])

    loads = [
        pltpu.make_async_copy(jacobian, blocks, load_sem.at[1]),
        pltpu.make_async_copy(source, rhs, load_sem.at[2]),
        pltpu.make_async_copy(couplings, weights_in, load_sem.at[3]),
        pltpu.make_async_copy(omega, speed_in, load_sem.at[4]),
    ]

    def remote(source_ref, target_ref, send, recv, **where):
        return pltpu.make_async_remote_copy(
            source_ref, target_ref, send, recv, device_id=where, device_id_type=MESH)

    def to_peer(k, x):
        recv = first_recv.at[0] if k == 0 else peer_recv.at[k - 1, x]
        return remote(cur.at[k, x + 1], peer.at[k, x], core_send.at[0], recv, inst=partner)

    def to_pair(k, x, hop):
        target = ((pair + hop) % pairs) * 2 + core
        outgoing = cur.at[0, x + 1] if k == 0 else part.at[k - 1, hop - 1, x]
        return remote(
            outgoing, got.at[k, hop - 1, x], x_send.at[0], got_recv.at[k % 2, hop - 1, x],
            inst=target)

    def relay(x, hop):
        return remote(
            got.at[0, hop - 1, x], relayed.at[hop - 1, x], core_send.at[1],
            relay_recv.at[hop - 1, x], inst=partner)

    def to_side(k, x, side):
        return remote(
            edge_out.at[k, x, side], edge_in.at[k, x, side], edge_send.at[0],
            edge_recv.at[k % 2, x], gy=up if side == 0 else down)

    def both_sides(k, x):
        return remote(
            edge_out.at[k, x], edge_in.at[k, x], edge_send.at[0], edge_recv.at[k % 2, x], gy=up)

    def to_next(k):
        return remote(
            cur.at[k, planes], cur.at[k, 0], side_send.at[0], side_recv.at[0, k], gx=at_x + 1)

    def to_last(k):
        return remote(
            cur.at[k, 1], cur.at[k, planes + 1], side_send.at[1], side_recv.at[1, k],
            gx=at_x - 1)

    def send_planes(k, x):
        to_peer(k, x).start()

        @pl.when(jnp.logical_and(x == planes - 1, has_high))
        def _():
            to_next(k).start()

        @pl.when(jnp.logical_and(x == 0, has_low))
        def _():
            to_last(k).start()

    def send_edges(k, x, field):
        for n in range(local):
            for v in range(nvar):
                at = n * nvar + v
                edge_out[k, x, 1, at:at + 1] = field[n][v][:1]
                edge_out[k, x, 0, at:at + 1] = field[n][v][rows - 1:]

    def start_edges(k, x):
        to_side(k, x, 0).start()
        to_side(k, x, 1).start()

    def mine(k, x):
        return [[cur[k, x + 1, n, v] for v in range(nvar)] for n in range(local)]

    even = core == 0

    def weights_of(hop, a):
        own = [derivative(2 * local * hop + a - b, total) for b in range(local)]
        other = [
            jnp.where(
                even,
                jnp.float32(derivative(2 * local * hop - local + a - b, total)),
                jnp.float32(derivative(2 * local * hop + local + a - b, total)),
            )
            for b in range(local)
        ]
        return own + other

    def send_parts(k, x):
        to_peer(k, x).wait_recv()
        for hop in hops:
            for a in range(local):
                weights = weights_of(hop, a)
                for v in range(nvar):
                    pieces = [cur[k, x + 1, b, v] for b in range(local)]
                    pieces += [peer[k, x, b, v] for b in range(local)]
                    part[k - 1, hop - 1, x, a, v] = weighted(weights, pieces)
            to_pair(k, x, hop).start()

    for step in range(planes):
        load_state(plane_of(step)).start()
    for copy in loads:
        copy.start()

    barrier = pltpu.get_barrier_semaphore()

    def greet(**where):
        pl.semaphore_signal(barrier, inc=1, device_id=where, device_id_type=MESH)

    leads = core == 1
    lead = pair * 2 + 1
    tail = pair * 2

    @pl.when(jnp.logical_not(leads))
    def _():
        greet(inst=lead)

    for hop in hops:
        greet(inst=((pair + hop) % pairs) * 2 + 1)
    greet(inst=tail, gy=up)
    greet(inst=tail, gy=down)

    @pl.when(has_low)
    def _():
        greet(inst=tail, gx=at_x - 1)

    @pl.when(has_high)
    def _():
        greet(inst=tail, gx=at_x + 1)

    zero = jnp.zeros((local, nvar, rows, depth), jnp.float32)

    @pl.when(jnp.logical_not(has_low))
    def _():
        for k in range(ITERS):
            cur[k, 0] = zero

    @pl.when(jnp.logical_not(has_high))
    def _():
        for k in range(ITERS):
            cur[k, planes + 1] = zero

    sides = has_low.astype(jnp.int32) + has_high.astype(jnp.int32)
    held = cur.at[0, 1:planes + 1]
    pltpu.make_async_copy(held, held, load_sem.at[0]).wait()

    def tell_partner():
        pl.semaphore_signal(
            ready.at[0], inc=1, device_id={"inst": partner}, device_id_type=MESH)

    @pl.when(leads)
    def _():
        pl.semaphore_wait(barrier, 2 * pairs - 1)
        tell_partner()

    @pl.when(jnp.logical_not(leads))
    def _():
        pl.semaphore_wait(ready.at[0], 1)

    @pl.loop(0, planes)
    def _(step):
        x = plane_of(step)
        for hop in hops:
            to_pair(0, x, hop).start()

    @pl.when(leads)
    def _():
        pl.semaphore_wait(ready.at[0], 1)

    @pl.when(jnp.logical_not(leads))
    def _():
        pl.semaphore_wait(barrier, 4 + 2 * sides)
        tell_partner()

    @pl.loop(0, planes)
    def _(step):
        x = plane_of(step)
        send_edges(0, x, mine(0, x))
        send_planes(0, x)
        start_edges(0, x)

    for copy in loads:
        copy.wait()

    @pl.loop(0, planes)
    def _(step):
        x = plane_of(step)
        for n in range(local):
            matrix = factor([[blocks[n, v, w, x] for w in range(nvar)] for v in range(nvar)])
            for v in range(nvar):
                for w in range(nvar):
                    lu[n, v, w, x] = matrix[v][w]

    row_at = lax.broadcasted_iota(jnp.int32, (rows, depth), 0)
    lane_at = lax.broadcasted_iota(jnp.int32, (rows, depth), 1)
    first_row, final_row = row_at == 0, row_at == rows - 1
    first_lane, final_lane = lane_at == 0, lane_at == depth - 1
    speed = speed_in[0]
    lag = min(LAG, planes)

    def near_side(k, x):
        result = [[None] * nvar for _ in range(local)]
        for w in range(nvar):
            for n in range(local):
                field = cur[k, x + 1, n, w]
                at = n * nvar + w
                shifted = [
                    cur[k, x, n, w],
                    cur[k, x + 2, n, w],
                    jnp.where(first_row, edge_in[k, x, 0, at:at + 1], pltpu.roll(field, 1, 0)),
                    jnp.where(
                        final_row, edge_in[k, x, 1, at:at + 1], pltpu.roll(field, rows - 1, 0)),
                    jnp.where(first_lane, 0.0, pltpu.roll(field, 1, 1)),
                    jnp.where(final_lane, 0.0, pltpu.roll(field, depth - 1, 1)),
                ]
                for v in range(nvar):
                    term = weighted([weights_in[v, d, w] for d in range(6)], shifted)
                    last = result[n][v]
                    result[n][v] = term if last is None else last + term
        for n in range(local):
            weights = weights_of(0, n)
            for v in range(nvar):
                pieces = [cur[k, x + 1, b, v] for b in range(local)]
                pieces += [peer[k, x, b, v] for b in range(local)]
                spectral = weighted(weights, pieces)
                result[n][v] = rhs[n, v, x] - result[n][v] - speed * spectral
        return result

    def far_side(k, x, n, v):
        spectral = None
        for hop in hops:
            if k == 0:
                pieces = [got[k, hop - 1, x, b, v] for b in range(local)]
                pieces += [relayed[hop - 1, x, b, v] for b in range(local)]
                term = weighted(weights_of(hop, n), pieces)
            else:
                term = got[k, hop - 1, x, n, v]
            spectral = term if spectral is None else spectral + term
        return spectral

    def pass_on(x):
        for hop in hops:
            to_pair(0, x, hop).wait_recv()
            relay(x, hop).start()

    pass_on(plane_of(0))
    pltpu.make_async_copy(peer.at[0], peer.at[0], first_recv.at[0]).wait()

    for k in range(ITERS):
        final_pass = k == ITERS - 1

        @pl.loop(0, planes)
        def _(step, k=k, final_pass=final_pass):
            x = plane_of(step)

            @pl.when(jnp.logical_and(x == 0, has_low))
            def _():
                to_next(k).wait_recv()

            @pl.when(jnp.logical_and(x == planes - 1, has_high))
            def _():
                to_last(k).wait_recv()

            both_sides(k, x).wait_recv()
            rights = near_side(k, x)
            if final_pass:
                own = mine(k, x)
                for n in range(local):
                    for v in range(nvar):
                        for w in range(nvar):
                            rights[n][v] = rights[n][v] - blocks[n, v, w, x] * own[n][w]
            if k == 0:

                @pl.when(step + 1 < planes)
                def _():
                    pass_on(plane_of(step + 1))

                for hop in hops:
                    relay(x, hop).wait_recv()
            else:
                for hop in hops:
                    to_pair(k, x, hop).wait_recv()
            fields = []
            for n in range(local):
                right = rights[n]
                if pairs > 1:
                    right = [right[v] - speed * far_side(k, x, n, v) for v in range(nvar)]
                answer = substitute(lambda v, w: lu[n, v, w, x], right)
                for v in range(nvar):
                    if final_pass:
                        last_residual[n, v, x] = right[v]
                        state_next[n, v, x] = own[n][v] + answer[v]
                    else:
                        cur[k + 1, x + 1, n, v] = answer[v]
                fields.append(answer)
            if not final_pass:
                send_edges(k + 1, x, fields)
                send_planes(k + 1, x)
                start_edges(k + 1, x)

                @pl.when(step >= lag)
                def _():
                    send_parts(k + 1, plane_of(step - lag))

            if k > 0:

                @pl.when(step < lag)
                def _():
                    send_parts(k, plane_of(planes - lag + step))

    for hop in hops:
        sent = got.at[:, hop - 1]
        remote(sent, sent, x_send.at[0], x_send.at[0], inst=partner).wait_send()
    remote(peer, peer, core_send.at[0], core_send.at[0], inst=partner).wait_send()
    remote(relayed, relayed, core_send.at[1], core_send.at[1], inst=partner).wait_send()
    remote(edge_out, edge_out, edge_send.at[0], edge_send.at[0], inst=partner).wait_send()
    layer = cur.at[:, 0]

    @pl.when(has_high)
    def _():
        remote(layer, layer, side_send.at[0], side_send.at[0], inst=partner).wait_send()

    @pl.when(has_low)
    def _():
        remote(layer, layer, side_send.at[1], side_send.at[1], inst=partner).wait_send()


def store(field, residual, state_next, last_residual, sems):
    copies = [
        pltpu.make_async_copy(field, state_next, sems.at[0]),
        pltpu.make_async_copy(residual, last_residual, sems.at[1]),
    ]
    for copy in copies:
        copy.start()
    for copy in copies:
        copy.wait()


def solution(mesh):
    ranks, count_x, count_y = mesh.shape["inst"], mesh.shape["gx"], mesh.shape["gy"]

    def shards(state, source, jacobian, couplings, omega):
        local, nvar, planes, rows, depth = state.shape
        pairs = ranks // 2
        cell = (local, nvar, rows, depth)
        edge = pltpu.VMEM((ITERS, planes, 2, local * nvar, depth), jnp.float32)
        hbm = pl.BlockSpec(memory_space=pltpu.HBM)
        near = pl.BlockSpec(memory_space=pltpu.VMEM)
        dma = pltpu.SemaphoreType.DMA
        vmem = lambda *lead: pltpu.VMEM(lead + cell, jnp.float32)
        matrices = pltpu.VMEM(jacobian.shape, jnp.float32)
        flows = couplings.transpose(1, 0, 2)
        field, residual = pl.pallas_call(
            functools.partial(kernel, ranks, count_x, count_y),
            out_shape=[pltpu.VMEM(state.shape, jnp.float32)] * 2,
            in_specs=[hbm] * 5,
            out_specs=[near, near],
            scratch_shapes=[
                vmem(ITERS, planes + 2), vmem(ITERS, planes),
                vmem(ITERS - 1, pairs - 1, planes), vmem(ITERS, pairs - 1, planes),
                vmem(pairs - 1, planes), edge, edge,
                pltpu.VMEM(state.shape, jnp.float32), matrices, matrices,
                pltpu.SMEM(flows.shape, jnp.float32), pltpu.SMEM(omega.shape, jnp.float32),
                dma((5,)), dma((1,)), dma((2,)), dma((1,)), dma((2,)),
                dma((1,)), dma((ITERS - 1, planes)), dma((pairs - 1, planes)),
                dma((2, pairs - 1, planes)), dma((2, planes)), dma((2, ITERS)),
                pltpu.SemaphoreType.REGULAR((1,)),
            ],
            compiler_params=pltpu.CompilerParams(
                collective_id=0, has_side_effects=True, vmem_limit_bytes=60 * 1024 * 1024),
            name="smooth",
        )(state, source, jacobian, flows, omega)
        return tuple(pl.pallas_call(
            store,
            out_shape=[jax.ShapeDtypeStruct(state.shape, jnp.float32)] * 2,
            in_specs=[near, near],
            out_specs=[hbm, hbm],
            scratch_shapes=[dma((2,))],
            compiler_params=pltpu.CompilerParams(vmem_limit_bytes=16 * 1024 * 1024),
            name="store",
        )(field, residual))

    split = P("inst", None, "gx", "gy", None)
    return jax.shard_map(
        shards,
        mesh=mesh,
        in_specs=(split, split, P("inst", None, None, "gx", "gy", None), P(), P()),
        out_specs=(split, split),
        check_vma=False,
    )
```

```python
import functools
import math

import jax
import jax.numpy as jnp
from jax import lax
from jax.experimental import pallas as pl
from jax.experimental.pallas import tpu as pltpu
from jax.sharding import PartitionSpec as P

ITERS = 3
LAG = 1
GROUP = 2
MESH = pl.DeviceIdType.MESH


def derivative(offset, total):
    offset = offset % total
    if offset > total // 2:
        offset -= total
    if offset == 0:
        return 0.0
    angle = math.pi * offset / total
    return 0.5 * (-1.0) ** offset * math.cos(angle) / math.sin(angle)


def factor(blocks):
    size = len(blocks)
    matrix = [list(row) for row in blocks]
    for pivot in range(size):
        matrix[pivot][pivot] = 1.0 / matrix[pivot][pivot]
        for target in range(pivot + 1, size):
            ratio = matrix[target][pivot] * matrix[pivot][pivot]
            matrix[target][pivot] = ratio
            for column in range(pivot + 1, size):
                matrix[target][column] = matrix[target][column] - ratio * matrix[pivot][column]
    return matrix


def substitute(matrix, right):
    size = len(right)
    vector = list(right)
    for pivot in range(size):
        for target in range(pivot + 1, size):
            vector[target] = vector[target] - matrix(target, pivot) * vector[pivot]
    result = [None] * size
    for pivot in reversed(range(size)):
        total = vector[pivot]
        for column in range(pivot + 1, size):
            total = total - matrix(pivot, column) * result[column]
        result[pivot] = total * matrix(pivot, pivot)
    return result


def weighted(weights, pieces):
    total = None
    for weight, piece in zip(weights, pieces):
        if isinstance(weight, float) and weight == 0.0:
            continue
        term = weight * piece
        total = term if total is None else total + term
    return total


def kernel(
    ranks, count_x, count_y,
    state, source, jacobian, couplings, omega,
    state_next, last_residual,
    cur, peer, part, got, edge_out, edge_in,
    cells, lu, weights_in, speed_in,
    load_sem, x_send, core_send, edge_send, side_send,
    first_recv, peer_recv, got_recv, edge_recv, side_recv, ready,
):
    local, nvar, planes, rows, depth = state.shape
    total = local * ranks
    pairs = ranks // 2
    rank = lax.axis_index("inst")
    at_x = lax.axis_index("gx")
    at_y = lax.axis_index("gy")
    pair = rank // 2
    core = rank % 2
    partner = pair * 2 + 1 - core
    up = (at_y + 1) % count_y
    down = (at_y + count_y - 1) % count_y
    has_low = at_x > 0
    has_high = at_x < count_x - 1
    flip = at_x % 2 == 0
    hops = range(1, pairs)
    group = GROUP if planes % GROUP == 0 else 1

    def plane_of(step):
        return jnp.where(flip, planes - 1 - step, step)

    def load_state(x):
        return pltpu.make_async_copy(state.at[:, :, x], cur.at[0, x + 1], load_sem.at[0])

    loads = [
        pltpu.make_async_copy(jacobian, cells.at[:, :, :nvar], load_sem.at[1]),
        pltpu.make_async_copy(source, cells.at[:, :, nvar], load_sem.at[1]),
        pltpu.make_async_copy(couplings, weights_in, load_sem.at[2]),
        pltpu.make_async_copy(omega, speed_in, load_sem.at[3]),
    ]

    def remote(source_ref, target_ref, send, recv, **where):
        return pltpu.make_async_remote_copy(
            source_ref, target_ref, send, recv, device_id=where, device_id_type=MESH)

    def to_peer(k, x):
        recv = first_recv.at[0] if k == 0 else peer_recv.at[k - 1, x]
        return remote(cur.at[k, x + 1], peer.at[k, x], core_send.at[0], recv, inst=partner)

    def to_pair(k, x, hop):
        target = ((pair + hop) % pairs) * 2 + core
        outgoing = cur.at[0, x + 1] if k == 0 else part.at[k - 1, hop - 1, x]
        return remote(
            outgoing, got.at[k, hop - 1, x], x_send.at[0], got_recv.at[k % 2, hop - 1, x],
            inst=target)

    def relay(x, hop):
        return remote(
            got.at[0, hop - 1, x], peer.at[ITERS + hop - 1, x], core_send.at[0],
            peer_recv.at[1 if hop == 1 else ITERS + hop - 3, x], inst=partner)

    def to_side(k, x, side):
        return remote(
            edge_out.at[k, x, side], edge_in.at[k, x, side], edge_send.at[0],
            edge_recv.at[k % 2, x // group], gy=up if side == 0 else down)

    def both_sides(k, x):
        some = edge_in.at[k, :group]
        return remote(some, some, edge_send.at[0], edge_recv.at[k % 2, x // group], gy=up)

    def to_next(k):
        return remote(
            cur.at[k, planes], cur.at[k, 0], side_send.at[0], side_recv.at[0, k % 2], gx=at_x + 1)

    def to_last(k):
        return remote(
            cur.at[k, 1], cur.at[k, planes + 1], side_send.at[1], side_recv.at[1, k % 2],
            gx=at_x - 1)

    def send_planes(k, x):
        to_peer(k, x).start()

        @pl.when(jnp.logical_and(x == planes - 1, has_high))
        def _():
            to_next(k).start()

        @pl.when(jnp.logical_and(x == 0, has_low))
        def _():
            to_last(k).start()

    def send_edges(k, x, field):
        for n in range(local):
            for v in range(nvar):
                at = n * nvar + v
                edge_out[k, x, 1, at:at + 1] = field[n][v][:1]
                edge_out[k, x, 0, at:at + 1] = field[n][v][rows - 1:]

    def start_edges(k, x):
        to_side(k, x, 0).start()
        to_side(k, x, 1).start()

    def mine(k, x):
        return [[cur[k, x + 1, n, v] for v in range(nvar)] for n in range(local)]

    even = core == 0

    def weights_of(hop, a):
        own = [derivative(2 * local * hop + a - b, total) for b in range(local)]
        other = [
            jnp.where(
                even,
                jnp.float32(derivative(2 * local * hop - local + a - b, total)),
                jnp.float32(derivative(2 * local * hop + local + a - b, total)),
            )
            for b in range(local)
        ]
        return own + other

    def send_parts(k, x):
        to_peer(k, x).wait_recv()
        for hop in hops:
            for a in range(local):
                weights = weights_of(hop, a)
                for v in range(nvar):
                    pieces = [cur[k, x + 1, b, v] for b in range(local)]
                    pieces += [peer[k, x, b, v] for b in range(local)]
                    part[k - 1, hop - 1, x, a, v] = weighted(weights, pieces)
            to_pair(k, x, hop).start()

    barrier = pltpu.get_barrier_semaphore()

    def greet(**where):
        pl.semaphore_signal(barrier, inc=1, device_id=where, device_id_type=MESH)

    leads = core == 1
    lead = pair * 2 + 1
    tail = pair * 2

    @pl.when(jnp.logical_not(leads))
    def _():
        greet(inst=lead)

    for hop in hops:
        greet(inst=((pair + hop) % pairs) * 2 + 1)
    greet(inst=tail, gy=up)
    greet(inst=tail, gy=down)

    @pl.when(has_low)
    def _():
        greet(inst=lead, gx=at_x - 1)

    @pl.when(has_high)
    def _():
        greet(inst=lead, gx=at_x + 1)

    for step in range(planes):
        load_state(plane_of(step)).start()
    for copy in loads:
        copy.start()

    zero = jnp.zeros((local, nvar, rows, depth), jnp.float32)

    @pl.when(jnp.logical_not(has_low))
    def _():
        for k in range(ITERS):
            cur[k, 0] = zero

    @pl.when(jnp.logical_not(has_high))
    def _():
        for k in range(ITERS):
            cur[k, planes + 1] = zero

    sides = has_low.astype(jnp.int32) + has_high.astype(jnp.int32)
    held = cur.at[0, 1:planes + 1]
    pltpu.make_async_copy(held, held, load_sem.at[0]).wait()

    def tell_partner():
        pl.semaphore_signal(
            ready.at[0], inc=1, device_id={"inst": partner}, device_id_type=MESH)

    @pl.when(leads)
    def _():
        pl.semaphore_wait(barrier, 2 * pairs - 1 + 2 * sides)
        tell_partner()

    @pl.when(jnp.logical_not(leads))
    def _():
        pl.semaphore_wait(ready.at[0], 1)

    @pl.loop(0, planes)
    def _(step):
        x = plane_of(step)
        for hop in hops:
            to_pair(0, x, hop).start()
        send_planes(0, x)

    @pl.when(leads)
    def _():
        pl.semaphore_wait(ready.at[0], 1)

    @pl.when(jnp.logical_not(leads))
    def _():
        pl.semaphore_wait(barrier, 4)
        tell_partner()

    @pl.loop(0, planes)
    def _(step):
        x = plane_of(step)
        send_edges(0, x, mine(0, x))
        start_edges(0, x)

    pltpu.make_async_copy(cells, cells, load_sem.at[1]).wait()
    for copy in loads[2:]:
        copy.wait()

    @pl.loop(0, planes)
    def _(step):
        x = plane_of(step)
        for n in range(local):
            matrix = factor([[cells[n, v, w, x] for w in range(nvar)] for v in range(nvar)])
            for v in range(nvar):
                for w in range(nvar):
                    lu[n, v, w, x] = matrix[v][w]

    row_at = lax.broadcasted_iota(jnp.int32, (rows, depth), 0)
    lane_at = lax.broadcasted_iota(jnp.int32, (rows, depth), 1)
    first_row, final_row = row_at == 0, row_at == rows - 1
    first_lane, final_lane = lane_at == 0, lane_at == depth - 1
    speed = speed_in[0]
    lag = min(LAG, planes)

    def near_side(k, x):
        result = [[None] * nvar for _ in range(local)]
        for w in range(nvar):
            for n in range(local):
                field = cur[k, x + 1, n, w]
                at = n * nvar + w
                shifted = [
                    cur[k, x, n, w],
                    cur[k, x + 2, n, w],
                    jnp.where(first_row, edge_in[k, x, 0, at:at + 1], pltpu.roll(field, 1, 0)),
                    jnp.where(
                        final_row, edge_in[k, x, 1, at:at + 1], pltpu.roll(field, rows - 1, 0)),
                    jnp.where(first_lane, 0.0, pltpu.roll(field, 1, 1)),
                    jnp.where(final_lane, 0.0, pltpu.roll(field, depth - 1, 1)),
                ]
                for v in range(nvar):
                    term = weighted([weights_in[v, d, w] for d in range(6)], shifted)
                    last = result[n][v]
                    result[n][v] = term if last is None else last + term
        for n in range(local):
            weights = weights_of(0, n)
            for v in range(nvar):
                pieces = [cur[k, x + 1, b, v] for b in range(local)]
                pieces += [peer[k, x, b, v] for b in range(local)]
                spectral = weighted(weights, pieces)
                result[n][v] = cells[n, v, nvar, x] - result[n][v] - speed * spectral
        return result

    def far_side(k, x, n, v):
        spectral = None
        for hop in hops:
            if k == 0:
                pieces = [got[k, hop - 1, x, b, v] for b in range(local)]
                pieces += [peer[ITERS + hop - 1, x, b, v] for b in range(local)]
                term = weighted(weights_of(hop, n), pieces)
            else:
                term = got[k, hop - 1, x, n, v]
            spectral = term if spectral is None else spectral + term
        return spectral

    def pass_on(x):
        for hop in hops:
            to_pair(0, x, hop).wait_recv()
            relay(x, hop).start()

    pass_on(plane_of(0))
    pltpu.make_async_copy(peer.at[0], peer.at[0], first_recv.at[0]).wait()

    for k in range(ITERS):
        final_pass = k == ITERS - 1

        @pl.loop(0, planes)
        def _(step, k=k, final_pass=final_pass):
            x = plane_of(step)

            @pl.when(jnp.logical_and(x == 0, has_low))
            def _():
                to_next(k).wait_recv()

            @pl.when(jnp.logical_and(x == planes - 1, has_high))
            def _():
                to_last(k).wait_recv()

            @pl.when(step % group == 0)
            def _():
                both_sides(k, x).wait_recv()

            rights = near_side(k, x)
            if final_pass:
                own = mine(k, x)
                for n in range(local):
                    for v in range(nvar):
                        for w in range(nvar):
                            rights[n][v] = rights[n][v] - cells[n, v, w, x] * own[n][w]
            if k == 0:

                @pl.when(step + 1 < planes)
                def _():
                    pass_on(plane_of(step + 1))

                for hop in hops:
                    relay(x, hop).wait_recv()
            else:
                for hop in hops:
                    to_pair(k, x, hop).wait_recv()
            fields = []
            for n in range(local):
                right = rights[n]
                if pairs > 1:
                    right = [right[v] - speed * far_side(k, x, n, v) for v in range(nvar)]
                answer = substitute(lambda v, w: lu[n, v, w, x], right)
                for v in range(nvar):
                    if final_pass:
                        last_residual[n, v, x] = right[v]
                        state_next[n, v, x] = own[n][v] + answer[v]
                    else:
                        cur[k + 1, x + 1, n, v] = answer[v]
                fields.append(answer)
            if not final_pass:
                send_edges(k + 1, x, fields)
                send_planes(k + 1, x)
                start_edges(k + 1, x)

                @pl.when(step >= lag)
                def _():
                    send_parts(k + 1, plane_of(step - lag))

            if k > 0:

                @pl.when(step < lag)
                def _():
                    send_parts(k, plane_of(planes - lag + step))

    for hop in hops:
        sent = got.at[:, hop - 1]
        remote(sent, sent, x_send.at[0], x_send.at[0], inst=partner).wait_send()
    remote(peer, peer, core_send.at[0], core_send.at[0], inst=partner).wait_send()
    remote(edge_out, edge_out, edge_send.at[0], edge_send.at[0], inst=partner).wait_send()
    layer = cur.at[:, 0]

    @pl.when(has_high)
    def _():
        remote(layer, layer, side_send.at[0], side_send.at[0], inst=partner).wait_send()

    @pl.when(has_low)
    def _():
        remote(layer, layer, side_send.at[1], side_send.at[1], inst=partner).wait_send()


def store(field, residual, state_next, last_residual, sems):
    copies = [
        pltpu.make_async_copy(field, state_next, sems.at[0]),
        pltpu.make_async_copy(residual, last_residual, sems.at[1]),
    ]
    for copy in copies:
        copy.start()
    for copy in copies:
        copy.wait()


def solution(mesh):
    ranks, count_x, count_y = mesh.shape["inst"], mesh.shape["gx"], mesh.shape["gy"]

    def shards(state, source, jacobian, couplings, omega):
        local, nvar, planes, rows, depth = state.shape
        pairs = ranks // 2
        cell = (local, nvar, rows, depth)
        group = GROUP if planes % GROUP == 0 else 1
        edge = pltpu.VMEM((ITERS, planes, 2, local * nvar, depth), jnp.float32)
        hbm = pl.BlockSpec(memory_space=pltpu.HBM)
        near = pl.BlockSpec(memory_space=pltpu.VMEM)
        dma = pltpu.SemaphoreType.DMA
        vmem = lambda *lead: pltpu.VMEM(lead + cell, jnp.float32)
        matrices = pltpu.VMEM(jacobian.shape, jnp.float32)
        padded = (local, nvar, nvar + 1, planes, rows, depth)
        flows = couplings.transpose(1, 0, 2)
        field, residual = pl.pallas_call(
            functools.partial(kernel, ranks, count_x, count_y),
            out_shape=[pltpu.VMEM(state.shape, jnp.float32)] * 2,
            in_specs=[hbm] * 5,
            out_specs=[near, near],
            scratch_shapes=[
                vmem(ITERS, planes + 2), vmem(ITERS + pairs - 1, planes),
                vmem(ITERS - 1, pairs - 1, planes), vmem(ITERS, pairs - 1, planes),
                edge, edge, pltpu.VMEM(padded, jnp.float32), matrices,
                pltpu.SMEM(flows.shape, jnp.float32), pltpu.SMEM(omega.shape, jnp.float32),
                dma((4,)), dma((1,)), dma((1,)), dma((1,)), dma((2,)),
                dma((1,)), dma((ITERS - 1 + max(pairs - 2, 0), planes)),
                dma((2, pairs - 1, planes)), dma((2, planes // group)), dma((2, 2)),
                pltpu.SemaphoreType.REGULAR((1,)),
            ],
            compiler_params=pltpu.CompilerParams(
                collective_id=0, has_side_effects=True, vmem_limit_bytes=60 * 1024 * 1024),
            name="smooth",
        )(state, source, jacobian, flows, omega)
        return tuple(pl.pallas_call(
            store,
            out_shape=[jax.ShapeDtypeStruct(state.shape, jnp.float32)] * 2,
            in_specs=[near, near],
            out_specs=[hbm, hbm],
            scratch_shapes=[dma((2,))],
            compiler_params=pltpu.CompilerParams(vmem_limit_bytes=16 * 1024 * 1024),
            name="store",
        )(field, residual))

    split = P("inst", None, "gx", "gy", None)
    return jax.shard_map(
        shards,
        mesh=mesh,
        in_specs=(split, split, P("inst", None, None, "gx", "gy", None), P(), P()),
        out_specs=(split, split),
        check_vma=False,
    )
```

```python
import functools
import math

import jax
import jax.numpy as jnp
from jax import lax
from jax.experimental import pallas as pl
from jax.experimental.pallas import tpu as pltpu
from jax.sharding import PartitionSpec as P

ITERS = 3
LAG = 1
GROUP = 2
MESH = pl.DeviceIdType.MESH


def derivative(offset, total):
    offset = offset % total
    if offset > total // 2:
        offset -= total
    if offset == 0:
        return 0.0
    angle = math.pi * offset / total
    return 0.5 * (-1.0) ** offset * math.cos(angle) / math.sin(angle)


def factor(blocks):
    size = len(blocks)
    matrix = [list(row) for row in blocks]
    for pivot in range(size):
        matrix[pivot][pivot] = 1.0 / matrix[pivot][pivot]
        for target in range(pivot + 1, size):
            ratio = matrix[target][pivot] * matrix[pivot][pivot]
            matrix[target][pivot] = ratio
            for column in range(pivot + 1, size):
                matrix[target][column] = matrix[target][column] - ratio * matrix[pivot][column]
    return matrix


def substitute(matrix, right):
    size = len(right)
    vector = list(right)
    for pivot in range(size):
        for target in range(pivot + 1, size):
            vector[target] = vector[target] - matrix(target, pivot) * vector[pivot]
    result = [None] * size
    for pivot in reversed(range(size)):
        total = vector[pivot]
        for column in range(pivot + 1, size):
            total = total - matrix(pivot, column) * result[column]
        result[pivot] = total * matrix(pivot, pivot)
    return result


def weighted(weights, pieces):
    total = None
    for weight, piece in zip(weights, pieces):
        if isinstance(weight, float) and weight == 0.0:
            continue
        term = weight * piece
        total = term if total is None else total + term
    return total


def kernel(
    ranks, count_x, count_y,
    state, source, jacobian, couplings, omega,
    state_next, last_residual,
    cur, peer, part, got, edge_out, edge_in,
    cells, lu, weights_in, speed_in,
    load_sem, x_send, core_send, edge_send, side_send,
    first_recv, peer_recv, got_recv, edge_recv, side_recv, ready,
):
    local, nvar, planes, rows, depth = state.shape
    total = local * ranks
    pairs = ranks // 2
    rank = lax.axis_index("inst")
    at_x = lax.axis_index("gx")
    at_y = lax.axis_index("gy")
    pair = rank // 2
    core = rank % 2
    partner = pair * 2 + 1 - core
    up = (at_y + 1) % count_y
    down = (at_y + count_y - 1) % count_y
    has_low = at_x > 0
    has_high = at_x < count_x - 1
    flip = at_x % 2 == 0
    hops = range(1, pairs)
    group = GROUP if planes % GROUP == 0 else 1

    def plane_of(step):
        return jnp.where(flip, planes - 1 - step, step)

    def load_state(x):
        return pltpu.make_async_copy(state.at[:, :, x], cur.at[0, x + 1], load_sem.at[0])

    loads = [
        pltpu.make_async_copy(jacobian, cells.at[:, :, :nvar], load_sem.at[1]),
        pltpu.make_async_copy(source, cells.at[:, :, nvar], load_sem.at[1]),
        pltpu.make_async_copy(couplings, weights_in, load_sem.at[2]),
        pltpu.make_async_copy(omega, speed_in, load_sem.at[3]),
    ]

    def remote(source_ref, target_ref, send, recv, **where):
        return pltpu.make_async_remote_copy(
            source_ref, target_ref, send, recv, device_id=where, device_id_type=MESH)

    def to_peer(k, x):
        recv = first_recv.at[0] if k == 0 else peer_recv.at[k - 1, x]
        return remote(cur.at[k, x + 1], peer.at[k, x], core_send.at[0], recv, inst=partner)

    def to_pair(k, x, hop):
        target = ((pair + hop) % pairs) * 2 + core
        outgoing = cur.at[0, x + 1] if k == 0 else part.at[k - 1, hop - 1, x]
        return remote(
            outgoing, got.at[k, hop - 1, x], x_send.at[0], got_recv.at[k % 2, hop - 1, x],
            inst=target)

    def relay(x, hop):
        return remote(
            got.at[0, hop - 1, x], peer.at[ITERS + hop - 1, x], core_send.at[0],
            peer_recv.at[1 if hop == 1 else ITERS + hop - 3, x], inst=partner)

    def to_side(k, x, side):
        return remote(
            edge_out.at[k, x, side], edge_in.at[k, x, side], edge_send.at[0],
            edge_recv.at[k % 2, x // group], gy=up if side == 0 else down)

    def both_sides(k, x):
        some = edge_in.at[k, :group]
        return remote(some, some, edge_send.at[0], edge_recv.at[k % 2, x // group], gy=up)

    def to_next(k):
        return remote(
            cur.at[k, planes], cur.at[k, 0], side_send.at[0], side_recv.at[0, k % 2], gx=at_x + 1)

    def to_last(k):
        return remote(
            cur.at[k, 1], cur.at[k, planes + 1], side_send.at[1], side_recv.at[1, k % 2],
            gx=at_x - 1)

    def send_layers(k):
        @pl.when(has_high)
        def _():
            to_next(k).start()

        @pl.when(has_low)
        def _():
            to_last(k).start()

    def send_planes(k, x):
        to_peer(k, x).start()

        @pl.when(jnp.logical_and(x == planes - 1, has_high))
        def _():
            to_next(k).start()

        @pl.when(jnp.logical_and(x == 0, has_low))
        def _():
            to_last(k).start()

    def send_edges(k, x, field):
        for n in range(local):
            for v in range(nvar):
                at = n * nvar + v
                edge_out[k, x, 1, at:at + 1] = field[n][v][:1]
                edge_out[k, x, 0, at:at + 1] = field[n][v][rows - 1:]

    def start_edges(k, x):
        to_side(k, x, 0).start()
        to_side(k, x, 1).start()

    def mine(k, x):
        return [[cur[k, x + 1, n, v] for v in range(nvar)] for n in range(local)]

    even = core == 0

    def weights_of(hop, a):
        own = [derivative(2 * local * hop + a - b, total) for b in range(local)]
        other = [
            jnp.where(
                even,
                jnp.float32(derivative(2 * local * hop - local + a - b, total)),
                jnp.float32(derivative(2 * local * hop + local + a - b, total)),
            )
            for b in range(local)
        ]
        return own + other

    def send_parts(k, x):
        to_peer(k, x).wait_recv()
        for hop in hops:
            for a in range(local):
                weights = weights_of(hop, a)
                for v in range(nvar):
                    pieces = [cur[k, x + 1, b, v] for b in range(local)]
                    pieces += [peer[k, x, b, v] for b in range(local)]
                    part[k - 1, hop - 1, x, a, v] = weighted(weights, pieces)
            to_pair(k, x, hop).start()

    barrier = pltpu.get_barrier_semaphore()

    def greet(**where):
        pl.semaphore_signal(barrier, inc=1, device_id=where, device_id_type=MESH)

    leads = core == 1
    tail = pair * 2
    counts_inst = rank == ranks - 1
    counts_side = rank == 1

    @pl.when(jnp.logical_not(counts_inst))
    def _():
        greet(inst=ranks - 1)

    greet(inst=tail, gy=up)
    greet(inst=tail, gy=down)

    @pl.when(has_low)
    def _():
        greet(inst=1, gx=at_x - 1)

    @pl.when(has_high)
    def _():
        greet(inst=1, gx=at_x + 1)

    for step in range(planes):
        load_state(plane_of(step)).start()
    for copy in loads:
        copy.start()

    zero = jnp.zeros((local, nvar, rows, depth), jnp.float32)

    @pl.when(jnp.logical_not(has_low))
    def _():
        for k in range(ITERS):
            cur[k, 0] = zero

    @pl.when(jnp.logical_not(has_high))
    def _():
        for k in range(ITERS):
            cur[k, planes + 1] = zero

    sides = has_low.astype(jnp.int32) + has_high.astype(jnp.int32)
    held = cur.at[0, 1:planes + 1]

    def tell(stage, where):
        pl.semaphore_signal(
            ready.at[stage], inc=1, device_id={"inst": where}, device_id_type=MESH)

    def gather(stage, counts, arrivals, others):
        @pl.when(counts)
        def _():
            pl.semaphore_wait(barrier, arrivals)
            for where in others:
                tell(stage, where)

        @pl.when(jnp.logical_not(counts))
        def _():
            pl.semaphore_wait(ready.at[stage], 1)

    gather(0, counts_inst, ranks - 1, range(ranks - 1))
    pltpu.make_async_copy(held, held, load_sem.at[0]).wait()

    @pl.loop(0, planes)
    def _(step):
        x = plane_of(step)
        for hop in hops:
            to_pair(0, x, hop).start()
        to_peer(0, x).start()

    def first_layers():
        gather(1, counts_side, ranks * sides, [at for at in range(ranks) if at != 1])
        send_layers(0)

    @pl.when(at_y % 2 == 0)
    def _():
        first_layers()

    gather(2, jnp.logical_not(leads), 4, [partner])

    @pl.loop(0, planes)
    def _(step):
        x = plane_of(step)
        send_edges(0, x, mine(0, x))
        start_edges(0, x)

    @pl.when(at_y % 2 == 1)
    def _():
        first_layers()
    pltpu.make_async_copy(cells, cells, load_sem.at[1]).wait()
    for copy in loads[2:]:
        copy.wait()

    @pl.loop(0, planes)
    def _(step):
        x = plane_of(step)
        for n in range(local):
            matrix = factor([[cells[n, v, w, x] for w in range(nvar)] for v in range(nvar)])
            for v in range(nvar):
                for w in range(nvar):
                    lu[n, v, w, x] = matrix[v][w]

    row_at = lax.broadcasted_iota(jnp.int32, (rows, depth), 0)
    lane_at = lax.broadcasted_iota(jnp.int32, (rows, depth), 1)
    first_row, final_row = row_at == 0, row_at == rows - 1
    first_lane, final_lane = lane_at == 0, lane_at == depth - 1
    speed = speed_in[0]
    lag = min(LAG, planes)

    def near_side(k, x):
        result = [[None] * nvar for _ in range(local)]
        for w in range(nvar):
            for n in range(local):
                field = cur[k, x + 1, n, w]
                at = n * nvar + w
                shifted = [
                    cur[k, x, n, w],
                    cur[k, x + 2, n, w],
                    jnp.where(first_row, edge_in[k, x, 0, at:at + 1], pltpu.roll(field, 1, 0)),
                    jnp.where(
                        final_row, edge_in[k, x, 1, at:at + 1], pltpu.roll(field, rows - 1, 0)),
                    jnp.where(first_lane, 0.0, pltpu.roll(field, 1, 1)),
                    jnp.where(final_lane, 0.0, pltpu.roll(field, depth - 1, 1)),
                ]
                for v in range(nvar):
                    term = weighted([weights_in[v, d, w] for d in range(6)], shifted)
                    last = result[n][v]
                    result[n][v] = term if last is None else last + term
        for n in range(local):
            weights = weights_of(0, n)
            for v in range(nvar):
                pieces = [cur[k, x + 1, b, v] for b in range(local)]
                pieces += [peer[k, x, b, v] for b in range(local)]
                spectral = weighted(weights, pieces)
                result[n][v] = cells[n, v, nvar, x] - result[n][v] - speed * spectral
        return result

    def far_side(k, x, n, v):
        spectral = None
        for hop in hops:
            if k == 0:
                pieces = [got[k, hop - 1, x, b, v] for b in range(local)]
                pieces += [peer[ITERS + hop - 1, x, b, v] for b in range(local)]
                term = weighted(weights_of(hop, n), pieces)
            else:
                term = got[k, hop - 1, x, n, v]
            spectral = term if spectral is None else spectral + term
        return spectral

    def pass_on(x):
        for hop in hops:
            to_pair(0, x, hop).wait_recv()
            relay(x, hop).start()

    pass_on(plane_of(0))
    pltpu.make_async_copy(peer.at[0], peer.at[0], first_recv.at[0]).wait()

    for k in range(ITERS):
        final_pass = k == ITERS - 1

        @pl.loop(0, planes)
        def _(step, k=k, final_pass=final_pass):
            x = plane_of(step)

            @pl.when(jnp.logical_and(x == 0, has_low))
            def _():
                to_next(k).wait_recv()

            @pl.when(jnp.logical_and(x == planes - 1, has_high))
            def _():
                to_last(k).wait_recv()

            @pl.when(step % group == 0)
            def _():
                both_sides(k, x).wait_recv()

            rights = near_side(k, x)
            if final_pass:
                own = mine(k, x)
                for n in range(local):
                    for v in range(nvar):
                        for w in range(nvar):
                            rights[n][v] = rights[n][v] - cells[n, v, w, x] * own[n][w]
            if k == 0:

                @pl.when(step + 1 < planes)
                def _():
                    pass_on(plane_of(step + 1))

                for hop in hops:
                    relay(x, hop).wait_recv()
            else:
                for hop in hops:
                    to_pair(k, x, hop).wait_recv()
            fields = []
            for n in range(local):
                right = rights[n]
                if pairs > 1:
                    right = [right[v] - speed * far_side(k, x, n, v) for v in range(nvar)]
                answer = substitute(lambda v, w: lu[n, v, w, x], right)
                for v in range(nvar):
                    if final_pass:
                        last_residual[n, v, x] = right[v]
                        state_next[n, v, x] = own[n][v] + answer[v]
                    else:
                        cur[k + 1, x + 1, n, v] = answer[v]
                fields.append(answer)
            if not final_pass:
                send_edges(k + 1, x, fields)
                send_planes(k + 1, x)
                start_edges(k + 1, x)

                @pl.when(step >= lag)
                def _():
                    send_parts(k + 1, plane_of(step - lag))

            if k > 0:

                @pl.when(step < lag)
                def _():
                    send_parts(k, plane_of(planes - lag + step))

    for hop in hops:
        sent = got.at[:, hop - 1]
        remote(sent, sent, x_send.at[0], x_send.at[0], inst=partner).wait_send()
    remote(peer, peer, core_send.at[0], core_send.at[0], inst=partner).wait_send()
    remote(edge_out, edge_out, edge_send.at[0], edge_send.at[0], inst=partner).wait_send()
    layer = cur.at[:, 0]

    @pl.when(has_high)
    def _():
        remote(layer, layer, side_send.at[0], side_send.at[0], inst=partner).wait_send()

    @pl.when(has_low)
    def _():
        remote(layer, layer, side_send.at[1], side_send.at[1], inst=partner).wait_send()


def store(field, residual, state_next, last_residual, sems):
    copies = [
        pltpu.make_async_copy(field, state_next, sems.at[0]),
        pltpu.make_async_copy(residual, last_residual, sems.at[1]),
    ]
    for copy in copies:
        copy.start()
    for copy in copies:
        copy.wait()


def solution(mesh):
    ranks, count_x, count_y = mesh.shape["inst"], mesh.shape["gx"], mesh.shape["gy"]

    def shards(state, source, jacobian, couplings, omega):
        local, nvar, planes, rows, depth = state.shape
        pairs = ranks // 2
        cell = (local, nvar, rows, depth)
        group = GROUP if planes % GROUP == 0 else 1
        edge = pltpu.VMEM((ITERS, planes, 2, local * nvar, depth), jnp.float32)
        hbm = pl.BlockSpec(memory_space=pltpu.HBM)
        near = pl.BlockSpec(memory_space=pltpu.VMEM)
        dma = pltpu.SemaphoreType.DMA
        vmem = lambda *lead: pltpu.VMEM(lead + cell, jnp.float32)
        matrices = pltpu.VMEM(jacobian.shape, jnp.float32)
        padded = (local, nvar, nvar + 1, planes, rows, depth)
        flows = couplings.transpose(1, 0, 2)
        field, residual = pl.pallas_call(
            functools.partial(kernel, ranks, count_x, count_y),
            out_shape=[pltpu.VMEM(state.shape, jnp.float32)] * 2,
            in_specs=[hbm] * 5,
            out_specs=[near, near],
            scratch_shapes=[
                vmem(ITERS, planes + 2), vmem(ITERS + pairs - 1, planes),
                vmem(ITERS - 1, pairs - 1, planes), vmem(ITERS, pairs - 1, planes),
                edge, edge, pltpu.VMEM(padded, jnp.float32), matrices,
                pltpu.SMEM(flows.shape, jnp.float32), pltpu.SMEM(omega.shape, jnp.float32),
                dma((4,)), dma((1,)), dma((1,)), dma((1,)), dma((2,)),
                dma((1,)), dma((ITERS - 1 + max(pairs - 2, 0), planes)),
                dma((2, pairs - 1, planes)), dma((2, planes // group)), dma((2, 2)),
                pltpu.SemaphoreType.REGULAR((3,)),
            ],
            compiler_params=pltpu.CompilerParams(
                collective_id=0, has_side_effects=True, vmem_limit_bytes=60 * 1024 * 1024),
            name="smooth",
        )(state, source, jacobian, flows, omega)
        return tuple(pl.pallas_call(
            store,
            out_shape=[jax.ShapeDtypeStruct(state.shape, jnp.float32)] * 2,
            in_specs=[near, near],
            out_specs=[hbm, hbm],
            scratch_shapes=[dma((2,))],
            compiler_params=pltpu.CompilerParams(vmem_limit_bytes=16 * 1024 * 1024),
            name="store",
        )(field, residual))

    split = P("inst", None, "gx", "gy", None)
    return jax.shard_map(
        shards,
        mesh=mesh,
        in_specs=(split, split, P("inst", None, None, "gx", "gy", None), P(), P()),
        out_specs=(split, split),
        check_vma=False,
    )
```

```python
import functools
import math

import jax
import jax.numpy as jnp
from jax import lax
from jax.experimental import pallas as pl
from jax.experimental.pallas import tpu as pltpu
from jax.sharding import PartitionSpec as P

ITERS = 3
LAG = 1
GROUP = 2
MESH = pl.DeviceIdType.MESH


def derivative(offset, total):
    offset = offset % total
    if offset > total // 2:
        offset -= total
    if offset == 0:
        return 0.0
    angle = math.pi * offset / total
    return 0.5 * (-1.0) ** offset * math.cos(angle) / math.sin(angle)


def factor(blocks):
    size = len(blocks)
    matrix = [list(row) for row in blocks]
    for pivot in range(size):
        matrix[pivot][pivot] = 1.0 / matrix[pivot][pivot]
        for target in range(pivot + 1, size):
            ratio = matrix[target][pivot] * matrix[pivot][pivot]
            matrix[target][pivot] = ratio
            for column in range(pivot + 1, size):
                matrix[target][column] = matrix[target][column] - ratio * matrix[pivot][column]
    return matrix


def substitute(matrix, right):
    size = len(right)
    vector = list(right)
    for pivot in range(size):
        for target in range(pivot + 1, size):
            vector[target] = vector[target] - matrix(target, pivot) * vector[pivot]
    result = [None] * size
    for pivot in reversed(range(size)):
        total = vector[pivot]
        for column in range(pivot + 1, size):
            total = total - matrix(pivot, column) * result[column]
        result[pivot] = total * matrix(pivot, pivot)
    return result


def weighted(weights, pieces):
    total = None
    for weight, piece in zip(weights, pieces):
        if isinstance(weight, float) and weight == 0.0:
            continue
        term = weight * piece
        total = term if total is None else total + term
    return total


def kernel(
    ranks, count_x, count_y,
    state, source, jacobian, couplings, omega,
    state_next, last_residual,
    cur, peer, part, got, edge_out, edge_in,
    cells, lu, weights_in, speed_in,
    load_sem, x_send, core_send, edge_send, side_send,
    first_recv, peer_recv, got_recv, edge_recv, side_recv, ready,
):
    local, nvar, planes, rows, depth = state.shape
    total = local * ranks
    pairs = ranks // 2
    rank = lax.axis_index("inst")
    at_x = lax.axis_index("gx")
    at_y = lax.axis_index("gy")
    pair = rank // 2
    core = rank % 2
    partner = pair * 2 + 1 - core
    up = (at_y + 1) % count_y
    down = (at_y + count_y - 1) % count_y
    has_low = at_x > 0
    has_high = at_x < count_x - 1
    flip = at_x % 2 == 0
    hops = range(1, pairs)
    group = GROUP if planes % GROUP == 0 else 1

    def plane_of(step):
        return jnp.where(flip, planes - 1 - step, step)

    def load_state(x):
        return pltpu.make_async_copy(state.at[:, :, x], cur.at[0, x + 1], load_sem.at[0])

    loads = [
        pltpu.make_async_copy(jacobian, cells.at[:, :, :nvar], load_sem.at[1]),
        pltpu.make_async_copy(source, cells.at[:, :, nvar], load_sem.at[1]),
        pltpu.make_async_copy(couplings, weights_in, load_sem.at[2]),
        pltpu.make_async_copy(omega, speed_in, load_sem.at[3]),
    ]

    def remote(source_ref, target_ref, send, recv, **where):
        return pltpu.make_async_remote_copy(
            source_ref, target_ref, send, recv, device_id=where, device_id_type=MESH)

    def to_peer(k, x):
        recv = first_recv.at[0] if k == 0 else peer_recv.at[k - 1, x]
        return remote(cur.at[k, x + 1], peer.at[k, x], core_send.at[0], recv, inst=partner)

    def to_pair(k, x, hop):
        target = ((pair + hop) % pairs) * 2 + core
        outgoing = cur.at[0, x + 1] if k == 0 else part.at[k - 1, hop - 1, x]
        return remote(
            outgoing, got.at[k, hop - 1, x], x_send.at[0], got_recv.at[k % 2, hop - 1, x],
            inst=target)

    def relay(x, hop):
        return remote(
            got.at[0, hop - 1, x], peer.at[ITERS + hop - 1, x], core_send.at[0],
            peer_recv.at[1 if hop == 1 else ITERS + hop - 3, x], inst=partner)

    def to_side(k, x, side):
        return remote(
            edge_out.at[k, x, side], edge_in.at[k, x, side], edge_send.at[0],
            edge_recv.at[k % 2, x // group], gy=up if side == 0 else down)

    def both_sides(k, x):
        some = edge_in.at[k, :group]
        return remote(some, some, edge_send.at[0], edge_recv.at[k % 2, x // group], gy=up)

    def to_next(k):
        return remote(
            cur.at[k, planes], cur.at[k, 0], side_send.at[0], side_recv.at[0, k % 2], gx=at_x + 1)

    def to_last(k):
        return remote(
            cur.at[k, 1], cur.at[k, planes + 1], side_send.at[1], side_recv.at[1, k % 2],
            gx=at_x - 1)

    def send_layers(k):
        @pl.when(has_high)
        def _():
            to_next(k).start()

        @pl.when(has_low)
        def _():
            to_last(k).start()

    def send_planes(k, x):
        to_peer(k, x).start()

        @pl.when(jnp.logical_and(x == planes - 1, has_high))
        def _():
            to_next(k).start()

        @pl.when(jnp.logical_and(x == 0, has_low))
        def _():
            to_last(k).start()

    def send_edges(k, x, field):
        for n in range(local):
            for v in range(nvar):
                at = n * nvar + v
                edge_out[k, x, 1, at:at + 1] = field[n][v][:1]
                edge_out[k, x, 0, at:at + 1] = field[n][v][rows - 1:]

    def start_edges(k, x):
        to_side(k, x, 0).start()
        to_side(k, x, 1).start()

    def mine(k, x):
        return [[cur[k, x + 1, n, v] for v in range(nvar)] for n in range(local)]

    even = core == 0

    def weights_of(hop, a):
        own = [derivative(2 * local * hop + a - b, total) for b in range(local)]
        other = [
            jnp.where(
                even,
                jnp.float32(derivative(2 * local * hop - local + a - b, total)),
                jnp.float32(derivative(2 * local * hop + local + a - b, total)),
            )
            for b in range(local)
        ]
        return own + other

    def send_parts(k, x):
        to_peer(k, x).wait_recv()
        for hop in hops:
            for a in range(local):
                weights = weights_of(hop, a)
                for v in range(nvar):
                    pieces = [cur[k, x + 1, b, v] for b in range(local)]
                    pieces += [peer[k, x, b, v] for b in range(local)]
                    part[k - 1, hop - 1, x, a, v] = weighted(weights, pieces)
            to_pair(k, x, hop).start()

    barrier = pltpu.get_barrier_semaphore()

    def greet(**where):
        pl.semaphore_signal(barrier, inc=1, device_id=where, device_id_type=MESH)

    leads = core == 1
    tail = pair * 2
    counts_inst = rank == ranks - 1
    counts_side = rank == 1

    @pl.when(jnp.logical_not(counts_inst))
    def _():
        greet(inst=ranks - 1)

    greet(inst=tail, gy=up)
    greet(inst=tail, gy=down)

    @pl.when(has_low)
    def _():
        greet(inst=1, gx=at_x - 1)

    @pl.when(has_high)
    def _():
        greet(inst=1, gx=at_x + 1)

    for step in range(planes):
        load_state(plane_of(step)).start()
    for copy in loads:
        copy.start()

    zero = jnp.zeros((local, nvar, rows, depth), jnp.float32)

    @pl.when(jnp.logical_not(has_low))
    def _():
        for k in range(ITERS):
            cur[k, 0] = zero

    @pl.when(jnp.logical_not(has_high))
    def _():
        for k in range(ITERS):
            cur[k, planes + 1] = zero

    sides = has_low.astype(jnp.int32) + has_high.astype(jnp.int32)
    held = cur.at[0, 1:planes + 1]

    def tell(stage, where):
        pl.semaphore_signal(
            ready.at[stage], inc=1, device_id={"inst": where}, device_id_type=MESH)

    def gather(stage, counts, arrivals, others):
        @pl.when(counts)
        def _():
            pl.semaphore_wait(barrier, arrivals)
            for where in others:
                tell(stage, where)

        @pl.when(jnp.logical_not(counts))
        def _():
            pl.semaphore_wait(ready.at[stage], 1)

    gather(0, counts_inst, ranks - 1, range(ranks - 1))
    pltpu.make_async_copy(held, held, load_sem.at[0]).wait()

    @pl.loop(0, planes)
    def _(step):
        x = plane_of(step)
        for hop in hops:
            to_pair(0, x, hop).start()
        to_peer(0, x).start()

    def first_layers():
        gather(1, counts_side, ranks * sides, [at for at in range(ranks) if at != 1])
        send_layers(0)

    @pl.when(at_y % 2 == 0)
    def _():
        first_layers()

    gather(2, jnp.logical_not(leads), 4, [partner])

    @pl.loop(0, planes)
    def _(step):
        x = plane_of(step)
        send_edges(0, x, mine(0, x))
        start_edges(0, x)

    @pl.when(at_y % 2 == 1)
    def _():
        first_layers()
    pltpu.make_async_copy(cells, cells, load_sem.at[1]).wait()
    for copy in loads[2:]:
        copy.wait()

    @pl.loop(0, planes)
    def _(step):
        x = plane_of(step)
        for n in range(local):
            matrix = factor([[cells[n, v, w, x] for w in range(nvar)] for v in range(nvar)])
            for v in range(nvar):
                for w in range(nvar):
                    lu[n, v, w, x] = matrix[v][w]

    row_at = lax.broadcasted_iota(jnp.int32, (rows, depth), 0)
    lane_at = lax.broadcasted_iota(jnp.int32, (rows, depth), 1)
    first_row, final_row = row_at == 0, row_at == rows - 1
    first_lane, final_lane = lane_at == 0, lane_at == depth - 1
    speed = speed_in[0]
    def lag_of(k):
        return jnp.where(jnp.logical_and(leads, k == ITERS - 1), min(5, planes), min(LAG, planes))


    def near_side(k, x):
        result = [[None] * nvar for _ in range(local)]
        for w in range(nvar):
            for n in range(local):
                field = cur[k, x + 1, n, w]
                at = n * nvar + w
                shifted = [
                    cur[k, x, n, w],
                    cur[k, x + 2, n, w],
                    jnp.where(first_row, edge_in[k, x, 0, at:at + 1], pltpu.roll(field, 1, 0)),
                    jnp.where(
                        final_row, edge_in[k, x, 1, at:at + 1], pltpu.roll(field, rows - 1, 0)),
                    jnp.where(first_lane, 0.0, pltpu.roll(field, 1, 1)),
                    jnp.where(final_lane, 0.0, pltpu.roll(field, depth - 1, 1)),
                ]
                for v in range(nvar):
                    term = weighted([weights_in[v, d, w] for d in range(6)], shifted)
                    last = result[n][v]
                    result[n][v] = term if last is None else last + term
        for n in range(local):
            weights = weights_of(0, n)
            for v in range(nvar):
                pieces = [cur[k, x + 1, b, v] for b in range(local)]
                pieces += [peer[k, x, b, v] for b in range(local)]
                spectral = weighted(weights, pieces)
                result[n][v] = cells[n, v, nvar, x] - result[n][v] - speed * spectral
        return result

    def far_side(k, x, n, v):
        spectral = None
        for hop in hops:
            if k == 0:
                pieces = [got[k, hop - 1, x, b, v] for b in range(local)]
                pieces += [peer[ITERS + hop - 1, x, b, v] for b in range(local)]
                term = weighted(weights_of(hop, n), pieces)
            else:
                term = got[k, hop - 1, x, n, v]
            spectral = term if spectral is None else spectral + term
        return spectral

    def pass_on(x):
        for hop in hops:
            to_pair(0, x, hop).wait_recv()
            relay(x, hop).start()

    pass_on(plane_of(0))
    pltpu.make_async_copy(peer.at[0], peer.at[0], first_recv.at[0]).wait()

    for k in range(ITERS):
        final_pass = k == ITERS - 1

        @pl.loop(0, planes)
        def _(step, k=k, final_pass=final_pass):
            x = plane_of(step)

            @pl.when(jnp.logical_and(x == 0, has_low))
            def _():
                to_next(k).wait_recv()

            @pl.when(jnp.logical_and(x == planes - 1, has_high))
            def _():
                to_last(k).wait_recv()

            @pl.when(step % group == 0)
            def _():
                both_sides(k, x).wait_recv()

            rights = near_side(k, x)
            if final_pass:
                own = mine(k, x)
                for n in range(local):
                    for v in range(nvar):
                        for w in range(nvar):
                            rights[n][v] = rights[n][v] - cells[n, v, w, x] * own[n][w]
            if k == 0:

                @pl.when(step + 1 < planes)
                def _():
                    pass_on(plane_of(step + 1))

                for hop in hops:
                    relay(x, hop).wait_recv()
            else:
                for hop in hops:
                    to_pair(k, x, hop).wait_recv()
            fields = []
            for n in range(local):
                right = rights[n]
                if pairs > 1:
                    right = [right[v] - speed * far_side(k, x, n, v) for v in range(nvar)]
                answer = substitute(lambda v, w: lu[n, v, w, x], right)
                for v in range(nvar):
                    if final_pass:
                        last_residual[n, v, x] = right[v]
                        state_next[n, v, x] = own[n][v] + answer[v]
                    else:
                        cur[k + 1, x + 1, n, v] = answer[v]
                fields.append(answer)
            if not final_pass:
                send_edges(k + 1, x, fields)
                send_planes(k + 1, x)
                start_edges(k + 1, x)

                later = lag_of(k + 1)

                @pl.when(step >= later)
                def _():
                    send_parts(k + 1, plane_of(step - later))

            if k > 0:
                now = lag_of(k)

                for j in range(2):
                    at = step * 2 + j

                    @pl.when(at < now)
                    def _(at=at):
                        send_parts(k, plane_of(planes - now + at))

    for hop in hops:
        sent = got.at[:, hop - 1]
        remote(sent, sent, x_send.at[0], x_send.at[0], inst=partner).wait_send()
    remote(peer, peer, core_send.at[0], core_send.at[0], inst=partner).wait_send()
    remote(edge_out, edge_out, edge_send.at[0], edge_send.at[0], inst=partner).wait_send()
    layer = cur.at[:, 0]

    @pl.when(has_high)
    def _():
        remote(layer, layer, side_send.at[0], side_send.at[0], inst=partner).wait_send()

    @pl.when(has_low)
    def _():
        remote(layer, layer, side_send.at[1], side_send.at[1], inst=partner).wait_send()


def store(field, residual, state_next, last_residual, sems):
    copies = [
        pltpu.make_async_copy(field, state_next, sems.at[0]),
        pltpu.make_async_copy(residual, last_residual, sems.at[1]),
    ]
    for copy in copies:
        copy.start()
    for copy in copies:
        copy.wait()


def solution(mesh):
    ranks, count_x, count_y = mesh.shape["inst"], mesh.shape["gx"], mesh.shape["gy"]

    def shards(state, source, jacobian, couplings, omega):
        local, nvar, planes, rows, depth = state.shape
        pairs = ranks // 2
        cell = (local, nvar, rows, depth)
        group = GROUP if planes % GROUP == 0 else 1
        edge = pltpu.VMEM((ITERS, planes, 2, local * nvar, depth), jnp.float32)
        hbm = pl.BlockSpec(memory_space=pltpu.HBM)
        near = pl.BlockSpec(memory_space=pltpu.VMEM)
        dma = pltpu.SemaphoreType.DMA
        vmem = lambda *lead: pltpu.VMEM(lead + cell, jnp.float32)
        matrices = pltpu.VMEM(jacobian.shape, jnp.float32)
        padded = (local, nvar, nvar + 1, planes, rows, depth)
        flows = couplings.transpose(1, 0, 2)
        field, residual = pl.pallas_call(
            functools.partial(kernel, ranks, count_x, count_y),
            out_shape=[pltpu.VMEM(state.shape, jnp.float32)] * 2,
            in_specs=[hbm] * 5,
            out_specs=[near, near],
            scratch_shapes=[
                vmem(ITERS, planes + 2), vmem(ITERS + pairs - 1, planes),
                vmem(ITERS - 1, pairs - 1, planes), vmem(ITERS, pairs - 1, planes),
                edge, edge, pltpu.VMEM(padded, jnp.float32), matrices,
                pltpu.SMEM(flows.shape, jnp.float32), pltpu.SMEM(omega.shape, jnp.float32),
                dma((4,)), dma((1,)), dma((1,)), dma((1,)), dma((2,)),
                dma((1,)), dma((ITERS - 1 + max(pairs - 2, 0), planes)),
                dma((2, pairs - 1, planes)), dma((2, planes // group)), dma((2, 2)),
                pltpu.SemaphoreType.REGULAR((3,)),
            ],
            compiler_params=pltpu.CompilerParams(
                collective_id=0, has_side_effects=True, vmem_limit_bytes=60 * 1024 * 1024),
            name="smooth",
        )(state, source, jacobian, flows, omega)
        return tuple(pl.pallas_call(
            store,
            out_shape=[jax.ShapeDtypeStruct(state.shape, jnp.float32)] * 2,
            in_specs=[near, near],
            out_specs=[hbm, hbm],
            scratch_shapes=[dma((2,))],
            compiler_params=pltpu.CompilerParams(vmem_limit_bytes=16 * 1024 * 1024),
            name="store",
        )(field, residual))

    split = P("inst", None, "gx", "gy", None)
    return jax.shard_map(
        shards,
        mesh=mesh,
        in_specs=(split, split, P("inst", None, None, "gx", "gy", None), P(), P()),
        out_specs=(split, split),
        check_vma=False,
    )
```

```python
import functools
import math

import jax
import jax.numpy as jnp
from jax import lax
from jax.experimental import pallas as pl
from jax.experimental.pallas import tpu as pltpu
from jax.sharding import PartitionSpec as P

ITERS = 3
LAG = 1
GROUP = 2
MESH = pl.DeviceIdType.MESH


def derivative(offset, total):
    offset = offset % total
    if offset > total // 2:
        offset -= total
    if offset == 0:
        return 0.0
    angle = math.pi * offset / total
    return 0.5 * (-1.0) ** offset * math.cos(angle) / math.sin(angle)


def factor(blocks):
    size = len(blocks)
    matrix = [list(row) for row in blocks]
    for pivot in range(size):
        matrix[pivot][pivot] = 1.0 / matrix[pivot][pivot]
        for target in range(pivot + 1, size):
            ratio = matrix[target][pivot] * matrix[pivot][pivot]
            matrix[target][pivot] = ratio
            for column in range(pivot + 1, size):
                matrix[target][column] = matrix[target][column] - ratio * matrix[pivot][column]
    return matrix


def substitute(matrix, right):
    size = len(right)
    vector = list(right)
    for pivot in range(size):
        for target in range(pivot + 1, size):
            vector[target] = vector[target] - matrix(target, pivot) * vector[pivot]
    result = [None] * size
    for pivot in reversed(range(size)):
        total = vector[pivot]
        for column in range(pivot + 1, size):
            total = total - matrix(pivot, column) * result[column]
        result[pivot] = total * matrix(pivot, pivot)
    return result


def weighted(weights, pieces):
    total = None
    for weight, piece in zip(weights, pieces):
        if isinstance(weight, float) and weight == 0.0:
            continue
        term = weight * piece
        total = term if total is None else total + term
    return total


def kernel(
    ranks, count_x, count_y,
    state, source, jacobian, couplings, omega,
    state_next, last_residual,
    cur, peer, part, got, edge_out, edge_in,
    cells, lu, weights_in, speed_in,
    load_sem, x_send, core_send, edge_send, side_send,
    first_recv, plane_recv, edge_recv, side_recv, ready,
):
    local, nvar, planes, rows, depth = state.shape
    total = local * ranks
    pairs = ranks // 2
    rank = lax.axis_index("inst")
    at_x = lax.axis_index("gx")
    at_y = lax.axis_index("gy")
    pair = rank // 2
    core = rank % 2
    partner = pair * 2 + 1 - core
    up = (at_y + 1) % count_y
    down = (at_y + count_y - 1) % count_y
    has_low = at_x > 0
    has_high = at_x < count_x - 1
    flip = at_x % 2 == 0
    hops = range(1, pairs)
    group = GROUP if planes % GROUP == 0 else 1

    def plane_of(step):
        return jnp.where(flip, planes - 1 - step, step)

    def load_state(x, at):
        return pltpu.make_async_copy(state.at[:, :, x], cur.at[0, x + 1], load_sem.at[at])

    loads = [
        pltpu.make_async_copy(jacobian, cells.at[:, :, :nvar], load_sem.at[1]),
        pltpu.make_async_copy(source, cells.at[:, :, nvar], load_sem.at[1]),
        pltpu.make_async_copy(couplings, weights_in, load_sem.at[2]),
        pltpu.make_async_copy(omega, speed_in, load_sem.at[3]),
    ]

    def remote(source_ref, target_ref, send, recv, **where):
        return pltpu.make_async_remote_copy(
            source_ref, target_ref, send, recv, device_id=where, device_id_type=MESH)

    def to_peer(k, x):
        recv = first_recv.at[0] if k == 0 else plane_recv.at[k - 1, x]
        return remote(cur.at[k, x + 1], peer.at[k, x], core_send.at[0], recv, inst=partner)

    def to_pair(k, x, hop):
        target = ((pair + hop) % pairs) * 2 + core
        outgoing = cur.at[0, x + 1] if k == 0 else part.at[k - 1, hop - 1, x]
        return remote(
            outgoing, got.at[k, hop - 1, x], x_send.at[0],
            plane_recv.at[3 * hop - 3 + 2 * (k % 2), x], inst=target)

    def relay(x, hop):
        return remote(
            got.at[0, hop - 1, x], peer.at[ITERS + hop - 1, x], core_send.at[0],
            plane_recv.at[3 * hop - 2, x], inst=partner)

    def to_side(k, x, side):
        return remote(
            edge_out.at[k, x, side], edge_in.at[k, x, side], edge_send.at[0],
            edge_recv.at[k % 2, x // group], gy=up if side == 0 else down)

    def both_sides(k, x):
        some = edge_in.at[k, :group]
        return remote(some, some, edge_send.at[0], edge_recv.at[k % 2, x // group], gy=up)

    def to_next(k):
        return remote(
            cur.at[k, planes], cur.at[k, 0], side_send.at[0], side_recv.at[0, k % 2], gx=at_x + 1)

    def to_last(k):
        return remote(
            cur.at[k, 1], cur.at[k, planes + 1], side_send.at[1], side_recv.at[1, k % 2],
            gx=at_x - 1)

    def send_layers(k):
        @pl.when(has_high)
        def _():
            to_next(k).start()

        @pl.when(has_low)
        def _():
            to_last(k).start()

    def send_planes(k, x):
        to_peer(k, x).start()

        @pl.when(jnp.logical_and(x == planes - 1, has_high))
        def _():
            to_next(k).start()

        @pl.when(jnp.logical_and(x == 0, has_low))
        def _():
            to_last(k).start()

    def send_edges(k, x, field):
        for n in range(local):
            for v in range(nvar):
                at = n * nvar + v
                edge_out[k, x, 1, at:at + 1] = field[n][v][:1]
                edge_out[k, x, 0, at:at + 1] = field[n][v][rows - 1:]

    def start_edges(k, x):
        to_side(k, x, 0).start()
        to_side(k, x, 1).start()

    def mine(k, x):
        return [[cur[k, x + 1, n, v] for v in range(nvar)] for n in range(local)]

    even = core == 0

    def weights_of(hop, a):
        own = [derivative(2 * local * hop + a - b, total) for b in range(local)]
        other = [
            jnp.where(
                even,
                jnp.float32(derivative(2 * local * hop - local + a - b, total)),
                jnp.float32(derivative(2 * local * hop + local + a - b, total)),
            )
            for b in range(local)
        ]
        return own + other

    def send_parts(k, x):
        to_peer(k, x).wait_recv()
        for hop in hops:
            for a in range(local):
                weights = weights_of(hop, a)
                for v in range(nvar):
                    pieces = [cur[k, x + 1, b, v] for b in range(local)]
                    pieces += [peer[k, x, b, v] for b in range(local)]
                    part[k - 1, hop - 1, x, a, v] = weighted(weights, pieces)
            to_pair(k, x, hop).start()

    for step in range(planes):
        load_state(plane_of(step), 0 if step == 0 else 4).start()

    barrier = pltpu.get_barrier_semaphore()

    def greet(**where):
        pl.semaphore_signal(barrier, inc=1, device_id=where, device_id_type=MESH)

    leads = core == 1
    tail = pair * 2
    counts_inst = rank == ranks - 1
    counts_side = rank == 1

    @pl.when(jnp.logical_not(counts_inst))
    def _():
        greet(inst=ranks - 1)

    greet(inst=tail, gy=up)
    greet(inst=tail, gy=down)

    @pl.when(has_low)
    def _():
        greet(inst=1, gx=at_x - 1)

    @pl.when(has_high)
    def _():
        greet(inst=1, gx=at_x + 1)

    for copy in loads:
        copy.start()

    zero = jnp.zeros((local, nvar, rows, depth), jnp.float32)

    @pl.when(jnp.logical_not(has_low))
    def _():
        for k in range(ITERS):
            cur[k, 0] = zero

    @pl.when(jnp.logical_not(has_high))
    def _():
        for k in range(ITERS):
            cur[k, planes + 1] = zero

    sides = has_low.astype(jnp.int32) + has_high.astype(jnp.int32)
    rest = cur.at[0, 1:planes]

    def tell(stage, where):
        pl.semaphore_signal(
            ready.at[stage], inc=1, device_id={"inst": where}, device_id_type=MESH)

    def gather(stage, counts, arrivals, others):
        @pl.when(counts)
        def _():
            pl.semaphore_wait(barrier, arrivals)
            for where in others:
                tell(stage, where)

        @pl.when(jnp.logical_not(counts))
        def _():
            pl.semaphore_wait(ready.at[stage], 1)

    gather(0, counts_inst, ranks - 1, range(ranks - 1))
    load_state(plane_of(0), 0).wait()

    for hop in hops:
        to_pair(0, plane_of(0), hop).start()

    pltpu.make_async_copy(rest, rest, load_sem.at[4]).wait()

    @pl.loop(1, planes)
    def _(step):
        for hop in hops:
            to_pair(0, plane_of(step), hop).start()

    @pl.loop(0, planes)
    def _(step):
        to_peer(0, plane_of(step)).start()

    def first_layers():
        gather(1, counts_side, ranks * sides, [at for at in range(ranks) if at != 1])
        send_layers(0)

    @pl.when(at_y % 2 == 0)
    def _():
        first_layers()

    gather(2, jnp.logical_not(leads), 4, [partner])

    @pl.loop(0, planes)
    def _(step):
        x = plane_of(step)
        send_edges(0, x, mine(0, x))
        start_edges(0, x)

    @pl.when(at_y % 2 == 1)
    def _():
        first_layers()
    pltpu.make_async_copy(cells, cells, load_sem.at[1]).wait()
    for copy in loads[2:]:
        copy.wait()

    @pl.loop(0, planes)
    def _(step):
        x = plane_of(step)
        for n in range(local):
            matrix = factor([[cells[n, v, w, x] for w in range(nvar)] for v in range(nvar)])
            for v in range(nvar):
                for w in range(nvar):
                    lu[n, v, w, x] = matrix[v][w]

    row_at = lax.broadcasted_iota(jnp.int32, (rows, depth), 0)
    lane_at = lax.broadcasted_iota(jnp.int32, (rows, depth), 1)
    first_row, final_row = row_at == 0, row_at == rows - 1
    first_lane, final_lane = lane_at == 0, lane_at == depth - 1
    speed = speed_in[0]
    def lag_of(k):
        return jnp.where(jnp.logical_and(leads, k == ITERS - 1), min(5, planes), min(LAG, planes))


    def near_side(k, x):
        result = [[None] * nvar for _ in range(local)]
        for w in range(nvar):
            for n in range(local):
                field = cur[k, x + 1, n, w]
                at = n * nvar + w
                shifted = [
                    cur[k, x, n, w],
                    cur[k, x + 2, n, w],
                    jnp.where(first_row, edge_in[k, x, 0, at:at + 1], pltpu.roll(field, 1, 0)),
                    jnp.where(
                        final_row, edge_in[k, x, 1, at:at + 1], pltpu.roll(field, rows - 1, 0)),
                    jnp.where(first_lane, 0.0, pltpu.roll(field, 1, 1)),
                    jnp.where(final_lane, 0.0, pltpu.roll(field, depth - 1, 1)),
                ]
                for v in range(nvar):
                    term = weighted([weights_in[v, d, w] for d in range(6)], shifted)
                    last = result[n][v]
                    result[n][v] = term if last is None else last + term
        for n in range(local):
            weights = weights_of(0, n)
            for v in range(nvar):
                pieces = [cur[k, x + 1, b, v] for b in range(local)]
                pieces += [peer[k, x, b, v] for b in range(local)]
                spectral = weighted(weights, pieces)
                result[n][v] = cells[n, v, nvar, x] - result[n][v] - speed * spectral
        return result

    def far_side(k, x, n, v):
        spectral = None
        for hop in hops:
            if k == 0:
                pieces = [got[k, hop - 1, x, b, v] for b in range(local)]
                pieces += [peer[ITERS + hop - 1, x, b, v] for b in range(local)]
                term = weighted(weights_of(hop, n), pieces)
            else:
                term = got[k, hop - 1, x, n, v]
            spectral = term if spectral is None else spectral + term
        return spectral

    def pass_on(x):
        for hop in hops:
            to_pair(0, x, hop).wait_recv()
            relay(x, hop).start()

    pass_on(plane_of(0))
    pltpu.make_async_copy(peer.at[0], peer.at[0], first_recv.at[0]).wait()

    for k in range(ITERS):
        final_pass = k == ITERS - 1

        @pl.loop(0, planes)
        def _(step, k=k, final_pass=final_pass):
            x = plane_of(step)

            @pl.when(jnp.logical_and(x == 0, has_low))
            def _():
                to_next(k).wait_recv()

            @pl.when(jnp.logical_and(x == planes - 1, has_high))
            def _():
                to_last(k).wait_recv()

            @pl.when(step % group == 0)
            def _():
                both_sides(k, x).wait_recv()

            rights = near_side(k, x)
            if final_pass:
                own = mine(k, x)
                for n in range(local):
                    for v in range(nvar):
                        for w in range(nvar):
                            rights[n][v] = rights[n][v] - cells[n, v, w, x] * own[n][w]
            if k == 0:

                @pl.when(step + 1 < planes)
                def _():
                    pass_on(plane_of(step + 1))

                for hop in hops:
                    relay(x, hop).wait_recv()
            else:
                for hop in hops:
                    to_pair(k, x, hop).wait_recv()
            fields = []
            for n in range(local):
                right = rights[n]
                if pairs > 1:
                    right = [right[v] - speed * far_side(k, x, n, v) for v in range(nvar)]
                answer = substitute(lambda v, w: lu[n, v, w, x], right)
                for v in range(nvar):
                    if final_pass:
                        last_residual[n, v, x] = right[v]
                        state_next[n, v, x] = own[n][v] + answer[v]
                    else:
                        cur[k + 1, x + 1, n, v] = answer[v]
                fields.append(answer)
            if not final_pass:
                send_edges(k + 1, x, fields)
                send_planes(k + 1, x)
                start_edges(k + 1, x)

                later = lag_of(k + 1)

                @pl.when(step >= later)
                def _():
                    send_parts(k + 1, plane_of(step - later))

            if k > 0:
                now = lag_of(k)

                for j in range(2):
                    at = step * 2 + j

                    @pl.when(at < now)
                    def _(at=at):
                        send_parts(k, plane_of(planes - now + at))

    for hop in hops:
        sent = got.at[:, hop - 1]
        remote(sent, sent, x_send.at[0], x_send.at[0], inst=partner).wait_send()
    remote(peer, peer, core_send.at[0], core_send.at[0], inst=partner).wait_send()
    remote(edge_out, edge_out, edge_send.at[0], edge_send.at[0], inst=partner).wait_send()
    layer = cur.at[:, 0]

    @pl.when(has_high)
    def _():
        remote(layer, layer, side_send.at[0], side_send.at[0], inst=partner).wait_send()

    @pl.when(has_low)
    def _():
        remote(layer, layer, side_send.at[1], side_send.at[1], inst=partner).wait_send()


def store(field, residual, state_next, last_residual, sems):
    copies = [
        pltpu.make_async_copy(field, state_next, sems.at[0]),
        pltpu.make_async_copy(residual, last_residual, sems.at[1]),
    ]
    for copy in copies:
        copy.start()
    for copy in copies:
        copy.wait()


def solution(mesh):
    ranks, count_x, count_y = mesh.shape["inst"], mesh.shape["gx"], mesh.shape["gy"]

    def shards(state, source, jacobian, couplings, omega):
        local, nvar, planes, rows, depth = state.shape
        pairs = ranks // 2
        cell = (local, nvar, rows, depth)
        group = GROUP if planes % GROUP == 0 else 1
        edge = pltpu.VMEM((ITERS, planes, 2, local * nvar, depth), jnp.float32)
        hbm = pl.BlockSpec(memory_space=pltpu.HBM)
        near = pl.BlockSpec(memory_space=pltpu.VMEM)
        dma = pltpu.SemaphoreType.DMA
        vmem = lambda *lead: pltpu.VMEM(lead + cell, jnp.float32)
        matrices = pltpu.VMEM(jacobian.shape, jnp.float32)
        padded = (local, nvar, nvar + 1, planes, rows, depth)
        flows = couplings.transpose(1, 0, 2)
        field, residual = pl.pallas_call(
            functools.partial(kernel, ranks, count_x, count_y),
            out_shape=[pltpu.VMEM(state.shape, jnp.float32)] * 2,
            in_specs=[hbm] * 5,
            out_specs=[near, near],
            scratch_shapes=[
                vmem(ITERS, planes + 2), vmem(ITERS + pairs - 1, planes),
                vmem(ITERS - 1, pairs - 1, planes), vmem(ITERS, pairs - 1, planes),
                edge, edge, pltpu.VMEM(padded, jnp.float32), matrices,
                pltpu.SMEM(flows.shape, jnp.float32), pltpu.SMEM(omega.shape, jnp.float32),
                dma((5,)), dma((1,)), dma((1,)), dma((1,)), dma((2,)),
                dma((1,)), dma((3 * (pairs - 1), planes)),
                dma((2, planes // group)), dma((2, 2)),
                pltpu.SemaphoreType.REGULAR((3,)),
            ],
            compiler_params=pltpu.CompilerParams(
                collective_id=0, has_side_effects=True, vmem_limit_bytes=60 * 1024 * 1024),
            name="smooth",
        )(state, source, jacobian, flows, omega)
        return tuple(pl.pallas_call(
            store,
            out_shape=[jax.ShapeDtypeStruct(state.shape, jnp.float32)] * 2,
            in_specs=[near, near],
            out_specs=[hbm, hbm],
            scratch_shapes=[dma((2,))],
            compiler_params=pltpu.CompilerParams(vmem_limit_bytes=16 * 1024 * 1024),
            name="store",
        )(field, residual))

    split = P("inst", None, "gx", "gy", None)
    return jax.shard_map(
        shards,
        mesh=mesh,
        in_specs=(split, split, P("inst", None, None, "gx", "gy", None), P(), P()),
        out_specs=(split, split),
        check_vma=False,
    )
```

```python
import functools
import math

import jax
import jax.numpy as jnp
from jax import lax
from jax.experimental import pallas as pl
from jax.experimental.pallas import tpu as pltpu
from jax.sharding import PartitionSpec as P

ITERS = 3
LAG = 1
GROUP = 2
MESH = pl.DeviceIdType.MESH


def derivative(offset, total):
    offset = offset % total
    if offset > total // 2:
        offset -= total
    if offset == 0:
        return 0.0
    angle = math.pi * offset / total
    return 0.5 * (-1.0) ** offset * math.cos(angle) / math.sin(angle)


def factor(blocks):
    size = len(blocks)
    matrix = [list(row) for row in blocks]
    for pivot in range(size):
        matrix[pivot][pivot] = 1.0 / matrix[pivot][pivot]
        for target in range(pivot + 1, size):
            ratio = matrix[target][pivot] * matrix[pivot][pivot]
            matrix[target][pivot] = ratio
            for column in range(pivot + 1, size):
                matrix[target][column] = matrix[target][column] - ratio * matrix[pivot][column]
    return matrix


def substitute(matrix, right):
    size = len(right)
    vector = list(right)
    for pivot in range(size):
        for target in range(pivot + 1, size):
            vector[target] = vector[target] - matrix(target, pivot) * vector[pivot]
    result = [None] * size
    for pivot in reversed(range(size)):
        total = vector[pivot]
        for column in range(pivot + 1, size):
            total = total - matrix(pivot, column) * result[column]
        result[pivot] = total * matrix(pivot, pivot)
    return result


def weighted(weights, pieces):
    total = None
    for weight, piece in zip(weights, pieces):
        if isinstance(weight, float) and weight == 0.0:
            continue
        term = weight * piece
        total = term if total is None else total + term
    return total


def kernel(
    ranks, count_x, count_y,
    state, source, jacobian, couplings, omega,
    state_next, last_residual,
    cur, peer, part, got, edge_out, edge_in,
    cells, lu, weights_in, speed_in,
    load_sem, x_send, core_send, edge_send, side_send,
    first_recv, plane_recv, edge_recv, side_recv, ready,
):
    local, nvar, planes, rows, depth = state.shape
    total = local * ranks
    pairs = ranks // 2
    rank = lax.axis_index("inst")
    at_x = lax.axis_index("gx")
    at_y = lax.axis_index("gy")
    pair = rank // 2
    core = rank % 2
    partner = pair * 2 + 1 - core
    up = (at_y + 1) % count_y
    down = (at_y + count_y - 1) % count_y
    has_low = at_x > 0
    has_high = at_x < count_x - 1
    flip = at_x % 2 == 0
    hops = range(1, pairs)
    group = GROUP if planes % GROUP == 0 else 1

    def plane_of(step):
        return jnp.where(flip, planes - 1 - step, step)

    def load_state(x, at):
        return pltpu.make_async_copy(state.at[:, :, x], cur.at[0, x + 1], load_sem.at[at])

    loads = [
        pltpu.make_async_copy(jacobian, cells.at[:, :, :nvar], load_sem.at[1]),
        pltpu.make_async_copy(source, cells.at[:, :, nvar], load_sem.at[1]),
        pltpu.make_async_copy(couplings, weights_in, load_sem.at[2]),
        pltpu.make_async_copy(omega, speed_in, load_sem.at[3]),
    ]

    def remote(source_ref, target_ref, send, recv, **where):
        return pltpu.make_async_remote_copy(
            source_ref, target_ref, send, recv, device_id=where, device_id_type=MESH)

    def to_peer(k, x):
        recv = first_recv.at[0] if k == 0 else plane_recv.at[k - 1, x]
        return remote(cur.at[k, x + 1], peer.at[k, x], core_send.at[0], recv, inst=partner)

    def to_pair(k, x, hop):
        target = ((pair + hop) % pairs) * 2 + core
        outgoing = cur.at[0, x + 1] if k == 0 else part.at[k - 1, hop - 1, x]
        return remote(
            outgoing, got.at[k, hop - 1, x], x_send.at[0],
            plane_recv.at[3 * hop - 3 + 2 * (k % 2), x], inst=target)

    def relay(x, hop):
        return remote(
            got.at[0, hop - 1, x], peer.at[ITERS + hop - 1, x], core_send.at[0],
            plane_recv.at[3 * hop - 2, x], inst=partner)

    def to_side(k, x, side):
        return remote(
            edge_out.at[k, x, side], edge_in.at[k, x, side], edge_send.at[0],
            edge_recv.at[k % 2, x // group], gy=up if side == 0 else down)

    def both_sides(k, x):
        some = edge_in.at[k, :group]
        return remote(some, some, edge_send.at[0], edge_recv.at[k % 2, x // group], gy=up)

    def to_next(k):
        return remote(
            cur.at[k, planes], cur.at[k, 0], side_send.at[0], side_recv.at[0, k % 2], gx=at_x + 1)

    def to_last(k):
        return remote(
            cur.at[k, 1], cur.at[k, planes + 1], side_send.at[1], side_recv.at[1, k % 2],
            gx=at_x - 1)

    def send_layers(k):
        @pl.when(has_high)
        def _():
            to_next(k).start()

        @pl.when(has_low)
        def _():
            to_last(k).start()

    def send_planes(k, x):
        to_peer(k, x).start()

        @pl.when(jnp.logical_and(x == planes - 1, has_high))
        def _():
            to_next(k).start()

        @pl.when(jnp.logical_and(x == 0, has_low))
        def _():
            to_last(k).start()

    def send_edges(k, x, field):
        for n in range(local):
            for v in range(nvar):
                at = n * nvar + v
                edge_out[k, x, 1, at:at + 1] = field[n][v][:1]
                edge_out[k, x, 0, at:at + 1] = field[n][v][rows - 1:]

    def start_edges(k, x):
        to_side(k, x, 0).start()
        to_side(k, x, 1).start()

    def mine(k, x):
        return [[cur[k, x + 1, n, v] for v in range(nvar)] for n in range(local)]

    even = core == 0

    def weights_of(hop, a):
        own = [derivative(2 * local * hop + a - b, total) for b in range(local)]
        other = [
            jnp.where(
                even,
                jnp.float32(derivative(2 * local * hop - local + a - b, total)),
                jnp.float32(derivative(2 * local * hop + local + a - b, total)),
            )
            for b in range(local)
        ]
        return own + other

    def send_parts(k, x):
        to_peer(k, x).wait_recv()
        for hop in hops:
            for a in range(local):
                weights = weights_of(hop, a)
                for v in range(nvar):
                    pieces = [cur[k, x + 1, b, v] for b in range(local)]
                    pieces += [peer[k, x, b, v] for b in range(local)]
                    part[k - 1, hop - 1, x, a, v] = weighted(weights, pieces)
            to_pair(k, x, hop).start()

    barrier = pltpu.get_barrier_semaphore()

    def greet(**where):
        pl.semaphore_signal(barrier, inc=1, device_id=where, device_id_type=MESH)

    leads = core == 1
    tail = pair * 2
    counts_inst = rank == ranks - 1
    counts_side = rank == 1

    @pl.when(jnp.logical_not(counts_inst))
    def _():
        greet(inst=ranks - 1)

    for step in range(planes):
        load_state(plane_of(step), 0 if step == 0 else 4).start()

    greet(inst=tail, gy=up)
    greet(inst=tail, gy=down)

    @pl.when(has_low)
    def _():
        greet(inst=1, gx=at_x - 1)

    @pl.when(has_high)
    def _():
        greet(inst=1, gx=at_x + 1)

    sides = has_low.astype(jnp.int32) + has_high.astype(jnp.int32)
    rest = cur.at[0, 1:planes]

    def tell(stage, where):
        pl.semaphore_signal(
            ready.at[stage], inc=1, device_id={"inst": where}, device_id_type=MESH)

    def gather(stage, counts, arrivals, others):
        @pl.when(counts)
        def _():
            pl.semaphore_wait(barrier, arrivals)
            for where in others:
                tell(stage, where)

        @pl.when(jnp.logical_not(counts))
        def _():
            pl.semaphore_wait(ready.at[stage], 1)

    gather(0, counts_inst, ranks - 1, range(ranks - 1))
    load_state(plane_of(0), 0).wait()

    for hop in hops:
        to_pair(0, plane_of(0), hop).start()

    pltpu.make_async_copy(rest, rest, load_sem.at[4]).wait()

    @pl.loop(1, planes)
    def _(step):
        for hop in hops:
            to_pair(0, plane_of(step), hop).start()

    for copy in loads:
        copy.start()

    @pl.loop(0, planes)
    def _(step):
        to_peer(0, plane_of(step)).start()

    zero = jnp.zeros((local, nvar, rows, depth), jnp.float32)

    @pl.when(jnp.logical_not(has_low))
    def _():
        for k in range(ITERS):
            cur[k, 0] = zero

    @pl.when(jnp.logical_not(has_high))
    def _():
        for k in range(ITERS):
            cur[k, planes + 1] = zero

    def first_layers():
        gather(1, counts_side, ranks * sides, [at for at in range(ranks) if at != 1])
        send_layers(0)

    @pl.when(at_y % 2 == 0)
    def _():
        first_layers()

    gather(2, jnp.logical_not(leads), 4, [partner])

    @pl.loop(0, planes)
    def _(step):
        x = plane_of(step)
        send_edges(0, x, mine(0, x))
        start_edges(0, x)

    @pl.when(at_y % 2 == 1)
    def _():
        first_layers()
    pltpu.make_async_copy(cells, cells, load_sem.at[1]).wait()
    for copy in loads[2:]:
        copy.wait()

    @pl.loop(0, planes)
    def _(step):
        x = plane_of(step)
        for n in range(local):
            matrix = factor([[cells[n, v, w, x] for w in range(nvar)] for v in range(nvar)])
            for v in range(nvar):
                for w in range(nvar):
                    lu[n, v, w, x] = matrix[v][w]

    row_at = lax.broadcasted_iota(jnp.int32, (rows, depth), 0)
    lane_at = lax.broadcasted_iota(jnp.int32, (rows, depth), 1)
    first_row, final_row = row_at == 0, row_at == rows - 1
    first_lane, final_lane = lane_at == 0, lane_at == depth - 1
    speed = speed_in[0]
    def lag_of(k):
        return jnp.where(jnp.logical_and(leads, k == ITERS - 1), min(5, planes), min(LAG, planes))


    def near_side(k, x):
        result = [[None] * nvar for _ in range(local)]
        for w in range(nvar):
            for n in range(local):
                field = cur[k, x + 1, n, w]
                at = n * nvar + w
                shifted = [
                    cur[k, x, n, w],
                    cur[k, x + 2, n, w],
                    jnp.where(first_row, edge_in[k, x, 0, at:at + 1], pltpu.roll(field, 1, 0)),
                    jnp.where(
                        final_row, edge_in[k, x, 1, at:at + 1], pltpu.roll(field, rows - 1, 0)),
                    jnp.where(first_lane, 0.0, pltpu.roll(field, 1, 1)),
                    jnp.where(final_lane, 0.0, pltpu.roll(field, depth - 1, 1)),
                ]
                for v in range(nvar):
                    term = weighted([weights_in[v, d, w] for d in range(6)], shifted)
                    last = result[n][v]
                    result[n][v] = term if last is None else last + term
        for n in range(local):
            weights = weights_of(0, n)
            for v in range(nvar):
                pieces = [cur[k, x + 1, b, v] for b in range(local)]
                pieces += [peer[k, x, b, v] for b in range(local)]
                spectral = weighted(weights, pieces)
                result[n][v] = cells[n, v, nvar, x] - result[n][v] - speed * spectral
        return result

    def far_side(k, x, n, v):
        spectral = None
        for hop in hops:
            if k == 0:
                pieces = [got[k, hop - 1, x, b, v] for b in range(local)]
                pieces += [peer[ITERS + hop - 1, x, b, v] for b in range(local)]
                term = weighted(weights_of(hop, n), pieces)
            else:
                term = got[k, hop - 1, x, n, v]
            spectral = term if spectral is None else spectral + term
        return spectral

    def pass_on(x):
        for hop in hops:
            to_pair(0, x, hop).wait_recv()
            relay(x, hop).start()

    pass_on(plane_of(0))
    pltpu.make_async_copy(peer.at[0], peer.at[0], first_recv.at[0]).wait()

    for k in range(ITERS):
        final_pass = k == ITERS - 1

        @pl.loop(0, planes)
        def _(step, k=k, final_pass=final_pass):
            x = plane_of(step)

            @pl.when(jnp.logical_and(x == 0, has_low))
            def _():
                to_next(k).wait_recv()

            @pl.when(jnp.logical_and(x == planes - 1, has_high))
            def _():
                to_last(k).wait_recv()

            @pl.when(step % group == 0)
            def _():
                both_sides(k, x).wait_recv()

            rights = near_side(k, x)
            if final_pass:
                own = mine(k, x)
                for n in range(local):
                    for v in range(nvar):
                        for w in range(nvar):
                            rights[n][v] = rights[n][v] - cells[n, v, w, x] * own[n][w]
            if k == 0:

                @pl.when(step + 1 < planes)
                def _():
                    pass_on(plane_of(step + 1))

                for hop in hops:
                    relay(x, hop).wait_recv()
            else:
                for hop in hops:
                    to_pair(k, x, hop).wait_recv()
            fields = []
            for n in range(local):
                right = rights[n]
                if pairs > 1:
                    right = [right[v] - speed * far_side(k, x, n, v) for v in range(nvar)]
                answer = substitute(lambda v, w: lu[n, v, w, x], right)
                for v in range(nvar):
                    if final_pass:
                        last_residual[n, v, x] = right[v]
                        state_next[n, v, x] = own[n][v] + answer[v]
                    else:
                        cur[k + 1, x + 1, n, v] = answer[v]
                fields.append(answer)
            if not final_pass:
                send_edges(k + 1, x, fields)
                send_planes(k + 1, x)
                start_edges(k + 1, x)

                later = lag_of(k + 1)

                @pl.when(step >= later)
                def _():
                    send_parts(k + 1, plane_of(step - later))

            if k > 0:
                now = lag_of(k)

                for j in range(2):
                    at = step * 2 + j

                    @pl.when(at < now)
                    def _(at=at):
                        send_parts(k, plane_of(planes - now + at))

    for hop in hops:
        sent = got.at[:, hop - 1]
        remote(sent, sent, x_send.at[0], x_send.at[0], inst=partner).wait_send()
    remote(peer, peer, core_send.at[0], core_send.at[0], inst=partner).wait_send()
    remote(edge_out, edge_out, edge_send.at[0], edge_send.at[0], inst=partner).wait_send()
    layer = cur.at[:, 0]

    @pl.when(has_high)
    def _():
        remote(layer, layer, side_send.at[0], side_send.at[0], inst=partner).wait_send()

    @pl.when(has_low)
    def _():
        remote(layer, layer, side_send.at[1], side_send.at[1], inst=partner).wait_send()


def store(field, residual, state_next, last_residual, sems):
    copies = [
        pltpu.make_async_copy(field, state_next, sems.at[0]),
        pltpu.make_async_copy(residual, last_residual, sems.at[1]),
    ]
    for copy in copies:
        copy.start()
    for copy in copies:
        copy.wait()


def solution(mesh):
    ranks, count_x, count_y = mesh.shape["inst"], mesh.shape["gx"], mesh.shape["gy"]

    def shards(state, source, jacobian, couplings, omega):
        local, nvar, planes, rows, depth = state.shape
        pairs = ranks // 2
        cell = (local, nvar, rows, depth)
        group = GROUP if planes % GROUP == 0 else 1
        edge = pltpu.VMEM((ITERS, planes, 2, local * nvar, depth), jnp.float32)
        hbm = pl.BlockSpec(memory_space=pltpu.HBM)
        near = pl.BlockSpec(memory_space=pltpu.VMEM)
        dma = pltpu.SemaphoreType.DMA
        vmem = lambda *lead: pltpu.VMEM(lead + cell, jnp.float32)
        matrices = pltpu.VMEM(jacobian.shape, jnp.float32)
        padded = (local, nvar, nvar + 1, planes, rows, depth)
        flows = couplings.transpose(1, 0, 2)
        field, residual = pl.pallas_call(
            functools.partial(kernel, ranks, count_x, count_y),
            out_shape=[pltpu.VMEM(state.shape, jnp.float32)] * 2,
            in_specs=[hbm] * 5,
            out_specs=[near, near],
            scratch_shapes=[
                vmem(ITERS, planes + 2), vmem(ITERS + pairs - 1, planes),
                vmem(ITERS - 1, pairs - 1, planes), vmem(ITERS, pairs - 1, planes),
                edge, edge, pltpu.VMEM(padded, jnp.float32), matrices,
                pltpu.SMEM(flows.shape, jnp.float32), pltpu.SMEM(omega.shape, jnp.float32),
                dma((5,)), dma((1,)), dma((1,)), dma((1,)), dma((2,)),
                dma((1,)), dma((3 * (pairs - 1), planes)),
                dma((2, planes // group)), dma((2, 2)),
                pltpu.SemaphoreType.REGULAR((3,)),
            ],
            compiler_params=pltpu.CompilerParams(
                collective_id=0, has_side_effects=True, vmem_limit_bytes=60 * 1024 * 1024),
            name="smooth",
        )(state, source, jacobian, flows, omega)
        return tuple(pl.pallas_call(
            store,
            out_shape=[jax.ShapeDtypeStruct(state.shape, jnp.float32)] * 2,
            in_specs=[near, near],
            out_specs=[hbm, hbm],
            scratch_shapes=[dma((2,))],
            compiler_params=pltpu.CompilerParams(vmem_limit_bytes=16 * 1024 * 1024),
            name="store",
        )(field, residual))

    split = P("inst", None, "gx", "gy", None)
    return jax.shard_map(
        shards,
        mesh=mesh,
        in_specs=(split, split, P("inst", None, None, "gx", "gy", None), P(), P()),
        out_specs=(split, split),
        check_vma=False,
    )
```

```python
import functools
import math

import jax
import jax.numpy as jnp
from jax import lax
from jax.experimental import pallas as pl
from jax.experimental.pallas import tpu as pltpu
from jax.sharding import PartitionSpec as P

ITERS = 3
LAG = 1
GROUP = 2
MESH = pl.DeviceIdType.MESH


def derivative(offset, total):
    offset = offset % total
    if offset > total // 2:
        offset -= total
    if offset == 0:
        return 0.0
    angle = math.pi * offset / total
    return 0.5 * (-1.0) ** offset * math.cos(angle) / math.sin(angle)


def factor(blocks):
    size = len(blocks)
    matrix = [list(row) for row in blocks]
    for pivot in range(size):
        matrix[pivot][pivot] = 1.0 / matrix[pivot][pivot]
        for target in range(pivot + 1, size):
            ratio = matrix[target][pivot] * matrix[pivot][pivot]
            matrix[target][pivot] = ratio
            for column in range(pivot + 1, size):
                matrix[target][column] = matrix[target][column] - ratio * matrix[pivot][column]
    return matrix


def substitute(matrix, right):
    size = len(right)
    vector = list(right)
    for pivot in range(size):
        for target in range(pivot + 1, size):
            vector[target] = vector[target] - matrix(target, pivot) * vector[pivot]
    result = [None] * size
    for pivot in reversed(range(size)):
        total = vector[pivot]
        for column in range(pivot + 1, size):
            total = total - matrix(pivot, column) * result[column]
        result[pivot] = total * matrix(pivot, pivot)
    return result


def weighted(weights, pieces):
    total = None
    for weight, piece in zip(weights, pieces):
        if isinstance(weight, float) and weight == 0.0:
            continue
        term = weight * piece
        total = term if total is None else total + term
    return total


def kernel(
    ranks, count_x, count_y,
    state, source, jacobian, couplings, omega,
    state_next, last_residual,
    cur, peer, part, got, edge_out, edge_in,
    cells, lu, weights_in, speed_in,
    load_sem, x_send, core_send, edge_send, side_send,
    first_recv, plane_recv, pair_recv, edge_recv, side_recv, ready,
):
    local, nvar, planes, rows, depth = state.shape
    total = local * ranks
    pairs = ranks // 2
    rank = lax.axis_index("inst")
    at_x = lax.axis_index("gx")
    at_y = lax.axis_index("gy")
    pair = rank // 2
    core = rank % 2
    partner = pair * 2 + 1 - core
    up = (at_y + 1) % count_y
    down = (at_y + count_y - 1) % count_y
    has_low = at_x > 0
    has_high = at_x < count_x - 1
    flip = at_x % 2 == 0
    hops = range(1, pairs)
    group = GROUP if planes % GROUP == 0 else 1

    def plane_of(step):
        return jnp.where(flip, planes - 1 - step, step)

    def load_state(x, at):
        return pltpu.make_async_copy(state.at[:, :, x], cur.at[0, x + 1], edge_recv.at[1, at])

    loads = [
        pltpu.make_async_copy(jacobian, cells.at[:, :, :nvar], load_sem.at[0]),
        pltpu.make_async_copy(source, cells.at[:, :, nvar], load_sem.at[0]),
        pltpu.make_async_copy(couplings, weights_in, load_sem.at[1]),
        pltpu.make_async_copy(omega, speed_in, load_sem.at[2]),
    ]

    def remote(source_ref, target_ref, send, recv, **where):
        return pltpu.make_async_remote_copy(
            source_ref, target_ref, send, recv, device_id=where, device_id_type=MESH)

    def to_peer(k, x):
        recv = first_recv.at[0] if k == 0 else plane_recv.at[k - 1, x]
        return remote(cur.at[k, x + 1], peer.at[k, x], core_send.at[0], recv, inst=partner)

    def got_recv(k, x, hop):
        if k % 2 == 1:
            return pair_recv.at[hop - 1, x // group]
        return plane_recv.at[2 * hop - 2, x]

    def to_pair(k, x, hop):
        target = ((pair + hop) % pairs) * 2 + core
        outgoing = cur.at[0, x + 1] if k == 0 else part.at[k - 1, hop - 1, x]
        return remote(
            outgoing, got.at[k, hop - 1, x], x_send.at[0],
            got_recv(k, x, hop), inst=target)

    def relay(x, hop):
        return remote(
            got.at[0, hop - 1, x], peer.at[ITERS + hop - 1, x], core_send.at[0],
            plane_recv.at[2 * hop - 1, x], inst=partner)

    def to_side(k, x, side):
        return remote(
            edge_out.at[k, x, side], edge_in.at[k, x, side], edge_send.at[0],
            edge_recv.at[k % 2, x // group], gy=up if side == 0 else down)

    def both_sides(k, x):
        some = edge_in.at[k, :group]
        return remote(some, some, edge_send.at[0], edge_recv.at[k % 2, x // group], gy=up)

    def to_next(k):
        return remote(
            cur.at[k, planes], cur.at[k, 0], side_send.at[0], side_recv.at[0, k % 2], gx=at_x + 1)

    def to_last(k):
        return remote(
            cur.at[k, 1], cur.at[k, planes + 1], side_send.at[1], side_recv.at[1, k % 2],
            gx=at_x - 1)

    def send_layers(k):
        @pl.when(has_high)
        def _():
            to_next(k).start()

        @pl.when(has_low)
        def _():
            to_last(k).start()

    def send_planes(k, x):
        to_peer(k, x).start()

        @pl.when(jnp.logical_and(x == planes - 1, has_high))
        def _():
            to_next(k).start()

        @pl.when(jnp.logical_and(x == 0, has_low))
        def _():
            to_last(k).start()

    def send_edges(k, x, field):
        for n in range(local):
            for v in range(nvar):
                at = n * nvar + v
                edge_out[k, x, 1, at:at + 1] = field[n][v][:1]
                edge_out[k, x, 0, at:at + 1] = field[n][v][rows - 1:]

    def start_edges(k, x):
        to_side(k, x, 0).start()
        to_side(k, x, 1).start()

    def mine(k, x):
        return [[cur[k, x + 1, n, v] for v in range(nvar)] for n in range(local)]

    even = core == 0

    def weights_of(hop, a):
        own = [derivative(2 * local * hop + a - b, total) for b in range(local)]
        other = [
            jnp.where(
                even,
                jnp.float32(derivative(2 * local * hop - local + a - b, total)),
                jnp.float32(derivative(2 * local * hop + local + a - b, total)),
            )
            for b in range(local)
        ]
        return own + other

    def send_parts(k, x):
        to_peer(k, x).wait_recv()
        for hop in hops:
            for a in range(local):
                weights = weights_of(hop, a)
                for v in range(nvar):
                    pieces = [cur[k, x + 1, b, v] for b in range(local)]
                    pieces += [peer[k, x, b, v] for b in range(local)]
                    part[k - 1, hop - 1, x, a, v] = weighted(weights, pieces)
            to_pair(k, x, hop).start()

    barrier = pltpu.get_barrier_semaphore()

    def greet(**where):
        pl.semaphore_signal(barrier, inc=1, device_id=where, device_id_type=MESH)

    leads = core == 1
    tail = pair * 2
    counts_inst = rank == ranks - 1
    counts_side = rank == 1

    @pl.when(jnp.logical_not(counts_inst))
    def _():
        greet(inst=ranks - 1)

    for step in range(planes):
        load_state(plane_of(step), min(step, 1)).start()

    greet(inst=tail, gy=up)
    greet(inst=tail, gy=down)

    @pl.when(has_low)
    def _():
        greet(inst=1, gx=at_x - 1)

    @pl.when(has_high)
    def _():
        greet(inst=1, gx=at_x + 1)

    sides = has_low.astype(jnp.int32) + has_high.astype(jnp.int32)
    rest = cur.at[0, 1:planes]

    def tell(stage, where):
        pl.semaphore_signal(
            ready.at[stage], inc=1, device_id={"inst": where}, device_id_type=MESH)

    def gather(stage, counts, arrivals, others):
        @pl.when(counts)
        def _():
            pl.semaphore_wait(barrier, arrivals)
            for where in others:
                tell(stage, where)

        @pl.when(jnp.logical_not(counts))
        def _():
            pl.semaphore_wait(ready.at[stage], 1)

    gather(0, counts_inst, ranks - 1, range(ranks - 1))
    load_state(plane_of(0), 0).wait()

    for hop in hops:
        to_pair(0, plane_of(0), hop).start()

    pltpu.make_async_copy(rest, rest, edge_recv.at[1, 1]).wait()

    @pl.loop(1, planes)
    def _(step):
        for hop in hops:
            to_pair(0, plane_of(step), hop).start()

    for copy in loads:
        copy.start()

    @pl.loop(0, planes)
    def _(step):
        to_peer(0, plane_of(step)).start()

    zero = jnp.zeros((local, nvar, rows, depth), jnp.float32)

    @pl.when(jnp.logical_not(has_low))
    def _():
        for k in range(ITERS):
            cur[k, 0] = zero

    @pl.when(jnp.logical_not(has_high))
    def _():
        for k in range(ITERS):
            cur[k, planes + 1] = zero

    def first_layers():
        gather(1, counts_side, ranks * sides, [at for at in range(ranks) if at != 1])
        send_layers(0)

    @pl.when(at_y % 2 == 0)
    def _():
        first_layers()

    gather(2, jnp.logical_not(leads), 4, [partner])

    @pl.loop(0, planes)
    def _(step):
        x = plane_of(step)
        send_edges(0, x, mine(0, x))
        start_edges(0, x)

    @pl.when(at_y % 2 == 1)
    def _():
        first_layers()
    pltpu.make_async_copy(cells, cells, load_sem.at[0]).wait()
    for copy in loads[2:]:
        copy.wait()

    @pl.loop(0, planes)
    def _(step):
        x = plane_of(step)
        for n in range(local):
            matrix = factor([[cells[n, v, w, x] for w in range(nvar)] for v in range(nvar)])
            for v in range(nvar):
                for w in range(nvar):
                    lu[n, v, w, x] = matrix[v][w]

    row_at = lax.broadcasted_iota(jnp.int32, (rows, depth), 0)
    lane_at = lax.broadcasted_iota(jnp.int32, (rows, depth), 1)
    first_row, final_row = row_at == 0, row_at == rows - 1
    first_lane, final_lane = lane_at == 0, lane_at == depth - 1
    speed = speed_in[0]
    def lag_of(k):
        return jnp.where(jnp.logical_and(leads, k == ITERS - 1), min(5, planes), min(LAG, planes))


    def near_side(k, x):
        result = [[None] * nvar for _ in range(local)]
        for w in range(nvar):
            for n in range(local):
                field = cur[k, x + 1, n, w]
                at = n * nvar + w
                shifted = [
                    cur[k, x, n, w],
                    cur[k, x + 2, n, w],
                    jnp.where(first_row, edge_in[k, x, 0, at:at + 1], pltpu.roll(field, 1, 0)),
                    jnp.where(
                        final_row, edge_in[k, x, 1, at:at + 1], pltpu.roll(field, rows - 1, 0)),
                    jnp.where(first_lane, 0.0, pltpu.roll(field, 1, 1)),
                    jnp.where(final_lane, 0.0, pltpu.roll(field, depth - 1, 1)),
                ]
                for v in range(nvar):
                    term = weighted([weights_in[v, d, w] for d in range(6)], shifted)
                    last = result[n][v]
                    result[n][v] = term if last is None else last + term
        for n in range(local):
            weights = weights_of(0, n)
            for v in range(nvar):
                pieces = [cur[k, x + 1, b, v] for b in range(local)]
                pieces += [peer[k, x, b, v] for b in range(local)]
                spectral = weighted(weights, pieces)
                result[n][v] = cells[n, v, nvar, x] - result[n][v] - speed * spectral
        return result

    def far_side(k, x, n, v):
        spectral = None
        for hop in hops:
            if k == 0:
                pieces = [got[k, hop - 1, x, b, v] for b in range(local)]
                pieces += [peer[ITERS + hop - 1, x, b, v] for b in range(local)]
                term = weighted(weights_of(hop, n), pieces)
            else:
                term = got[k, hop - 1, x, n, v]
            spectral = term if spectral is None else spectral + term
        return spectral

    def pass_on(x):
        for hop in hops:
            to_pair(0, x, hop).wait_recv()
            relay(x, hop).start()

    pass_on(plane_of(0))
    pltpu.make_async_copy(peer.at[0], peer.at[0], first_recv.at[0]).wait()

    for k in range(ITERS):
        final_pass = k == ITERS - 1

        @pl.loop(0, planes)
        def _(step, k=k, final_pass=final_pass):
            x = plane_of(step)

            @pl.when(jnp.logical_and(x == 0, has_low))
            def _():
                to_next(k).wait_recv()

            @pl.when(jnp.logical_and(x == planes - 1, has_high))
            def _():
                to_last(k).wait_recv()

            @pl.when(step % group == 0)
            def _():
                both_sides(k, x).wait_recv()

            rights = near_side(k, x)
            if final_pass:
                own = mine(k, x)
                for n in range(local):
                    for v in range(nvar):
                        for w in range(nvar):
                            rights[n][v] = rights[n][v] - cells[n, v, w, x] * own[n][w]
            if k == 0:

                @pl.when(step + 1 < planes)
                def _():
                    pass_on(plane_of(step + 1))

                for hop in hops:
                    relay(x, hop).wait_recv()
            else:
                for hop in hops:
                    if k % 2 == 0:
                        to_pair(k, x, hop).wait_recv()
                        continue

                    @pl.when(step % group == 0)
                    def _(hop=hop):
                        both = got.at[k, hop - 1, :group]
                        remote(
                            both, both, x_send.at[0], got_recv(k, x, hop),
                            inst=partner).wait_recv()
            fields = []
            for n in range(local):
                right = rights[n]
                if pairs > 1:
                    right = [right[v] - speed * far_side(k, x, n, v) for v in range(nvar)]
                answer = substitute(lambda v, w: lu[n, v, w, x], right)
                for v in range(nvar):
                    if final_pass:
                        last_residual[n, v, x] = right[v]
                        state_next[n, v, x] = own[n][v] + answer[v]
                    else:
                        cur[k + 1, x + 1, n, v] = answer[v]
                fields.append(answer)
            if not final_pass:
                send_edges(k + 1, x, fields)
                send_planes(k + 1, x)
                start_edges(k + 1, x)

                later = lag_of(k + 1)

                @pl.when(step >= later)
                def _():
                    send_parts(k + 1, plane_of(step - later))

            if k > 0:
                now = lag_of(k)

                for j in range(2):
                    at = step * 2 + j

                    @pl.when(at < now)
                    def _(at=at):
                        send_parts(k, plane_of(planes - now + at))

    for hop in hops:
        sent = got.at[:, hop - 1]
        remote(sent, sent, x_send.at[0], x_send.at[0], inst=partner).wait_send()
    remote(peer, peer, core_send.at[0], core_send.at[0], inst=partner).wait_send()
    remote(edge_out, edge_out, edge_send.at[0], edge_send.at[0], inst=partner).wait_send()
    layer = cur.at[:, 0]

    @pl.when(has_high)
    def _():
        remote(layer, layer, side_send.at[0], side_send.at[0], inst=partner).wait_send()

    @pl.when(has_low)
    def _():
        remote(layer, layer, side_send.at[1], side_send.at[1], inst=partner).wait_send()


def store(field, residual, state_next, last_residual, sems):
    copies = [
        pltpu.make_async_copy(field, state_next, sems.at[0]),
        pltpu.make_async_copy(residual, last_residual, sems.at[1]),
    ]
    for copy in copies:
        copy.start()
    for copy in copies:
        copy.wait()


def solution(mesh):
    ranks, count_x, count_y = mesh.shape["inst"], mesh.shape["gx"], mesh.shape["gy"]

    def shards(state, source, jacobian, couplings, omega):
        local, nvar, planes, rows, depth = state.shape
        pairs = ranks // 2
        cell = (local, nvar, rows, depth)
        group = GROUP if planes % GROUP == 0 else 1
        edge = pltpu.VMEM((ITERS, planes, 2, local * nvar, depth), jnp.float32)
        hbm = pl.BlockSpec(memory_space=pltpu.HBM)
        near = pl.BlockSpec(memory_space=pltpu.VMEM)
        dma = pltpu.SemaphoreType.DMA
        vmem = lambda *lead: pltpu.VMEM(lead + cell, jnp.float32)
        matrices = pltpu.VMEM(jacobian.shape, jnp.float32)
        padded = (local, nvar, nvar + 1, planes, rows, depth)
        flows = couplings.transpose(1, 0, 2)
        field, residual = pl.pallas_call(
            functools.partial(kernel, ranks, count_x, count_y),
            out_shape=[pltpu.VMEM(state.shape, jnp.float32)] * 2,
            in_specs=[hbm] * 5,
            out_specs=[near, near],
            scratch_shapes=[
                vmem(ITERS, planes + 2), vmem(ITERS + pairs - 1, planes),
                vmem(ITERS - 1, pairs - 1, planes), vmem(ITERS, pairs - 1, planes),
                edge, edge, pltpu.VMEM(padded, jnp.float32), matrices,
                pltpu.SMEM(flows.shape, jnp.float32), pltpu.SMEM(omega.shape, jnp.float32),
                dma((3,)), dma((1,)), dma((1,)), dma((1,)), dma((2,)),
                dma((1,)), dma((2 * (pairs - 1), planes)), dma((pairs - 1, planes // group)),
                dma((2, max(planes // group, 2))), dma((2, 2)),
                pltpu.SemaphoreType.REGULAR((3,)),
            ],
            compiler_params=pltpu.CompilerParams(
                collective_id=0, has_side_effects=True, vmem_limit_bytes=60 * 1024 * 1024),
            name="smooth",
        )(state, source, jacobian, flows, omega)
        return tuple(pl.pallas_call(
            store,
            out_shape=[jax.ShapeDtypeStruct(state.shape, jnp.float32)] * 2,
            in_specs=[near, near],
            out_specs=[hbm, hbm],
            scratch_shapes=[dma((2,))],
            compiler_params=pltpu.CompilerParams(vmem_limit_bytes=16 * 1024 * 1024),
            name="store",
        )(field, residual))

    split = P("inst", None, "gx", "gy", None)
    return jax.shard_map(
        shards,
        mesh=mesh,
        in_specs=(split, split, P("inst", None, None, "gx", "gy", None), P(), P()),
        out_specs=(split, split),
        check_vma=False,
    )
```

```python
import functools
import math

import jax
import jax.numpy as jnp
from jax import lax
from jax.experimental import pallas as pl
from jax.experimental.pallas import tpu as pltpu
from jax.sharding import PartitionSpec as P

ITERS = 3
LAG = 1
GROUP = 2
MESH = pl.DeviceIdType.MESH


def derivative(offset, total):
    offset = offset % total
    if offset > total // 2:
        offset -= total
    if offset == 0:
        return 0.0
    angle = math.pi * offset / total
    return 0.5 * (-1.0) ** offset * math.cos(angle) / math.sin(angle)


def factor(blocks):
    size = len(blocks)
    matrix = [list(row) for row in blocks]
    for pivot in range(size):
        matrix[pivot][pivot] = 1.0 / matrix[pivot][pivot]
        for target in range(pivot + 1, size):
            ratio = matrix[target][pivot] * matrix[pivot][pivot]
            matrix[target][pivot] = ratio
            for column in range(pivot + 1, size):
                matrix[target][column] = matrix[target][column] - ratio * matrix[pivot][column]
    return matrix


def substitute(matrix, right):
    size = len(right)
    vector = list(right)
    for pivot in range(size):
        for target in range(pivot + 1, size):
            vector[target] = vector[target] - matrix(target, pivot) * vector[pivot]
    result = [None] * size
    for pivot in reversed(range(size)):
        total = vector[pivot]
        for column in range(pivot + 1, size):
            total = total - matrix(pivot, column) * result[column]
        result[pivot] = total * matrix(pivot, pivot)
    return result


def weighted(weights, pieces):
    total = None
    for weight, piece in zip(weights, pieces):
        if isinstance(weight, float) and weight == 0.0:
            continue
        term = weight * piece
        total = term if total is None else total + term
    return total


def kernel(
    ranks, count_x, count_y,
    state, source, jacobian, couplings, omega,
    state_next, last_residual,
    cur, peer, part, got, edge_out, edge_in,
    cells, lu, weights_in, speed_in,
    load_sem, x_send, core_send, edge_send, side_send,
    first_recv, plane_recv, edge_recv, side_recv, ready,
):
    local, nvar, planes, rows, depth = state.shape
    total = local * ranks
    pairs = ranks // 2
    rank = lax.axis_index("inst")
    at_x = lax.axis_index("gx")
    at_y = lax.axis_index("gy")
    pair = rank // 2
    core = rank % 2
    partner = pair * 2 + 1 - core
    up = (at_y + 1) % count_y
    down = (at_y + count_y - 1) % count_y
    has_low = at_x > 0
    has_high = at_x < count_x - 1
    flip = at_x % 2 == 0
    hops = range(1, pairs)
    group = GROUP if planes % GROUP == 0 else 1

    def plane_of(step):
        return jnp.where(flip, planes - 1 - step, step)

    def load_state(x, at):
        return pltpu.make_async_copy(state.at[:, :, x], cur.at[0, x + 1], load_sem.at[at])

    loads = [
        pltpu.make_async_copy(jacobian, cells.at[:, :, :nvar], load_sem.at[1]),
        pltpu.make_async_copy(source, cells.at[:, :, nvar], load_sem.at[1]),
        pltpu.make_async_copy(couplings, weights_in, load_sem.at[2]),
        pltpu.make_async_copy(omega, speed_in, load_sem.at[3]),
    ]

    def remote(source_ref, target_ref, send, recv, **where):
        return pltpu.make_async_remote_copy(
            source_ref, target_ref, send, recv, device_id=where, device_id_type=MESH)

    def to_peer(k, x):
        recv = first_recv.at[0] if k == 0 else plane_recv.at[k - 1, x]
        return remote(cur.at[k, x + 1], peer.at[k, x], core_send.at[0], recv, inst=partner)

    def to_pair(k, x, hop):
        target = ((pair + hop) % pairs) * 2 + core
        outgoing = cur.at[0, x + 1] if k == 0 else part.at[k - 1, hop - 1, x]
        return remote(
            outgoing, got.at[k, hop - 1, x], x_send.at[0],
            plane_recv.at[3 * hop - 3 + 2 * (k % 2), x], inst=target)

    def relay(x, hop):
        return remote(
            got.at[0, hop - 1, x], peer.at[ITERS + hop - 1, x], core_send.at[0],
            plane_recv.at[3 * hop - 2, x], inst=partner)

    def to_side(k, x, side):
        return remote(
            edge_out.at[k, x, side], edge_in.at[k, x, side], edge_send.at[0],
            edge_recv.at[k % 2, x // group], gy=up if side == 0 else down)

    def both_sides(k, x):
        some = edge_in.at[k, :group]
        return remote(some, some, edge_send.at[0], edge_recv.at[k % 2, x // group], gy=up)

    def to_next(k):
        return remote(
            cur.at[k, planes], cur.at[k, 0], side_send.at[0], side_recv.at[0, k % 2], gx=at_x + 1)

    def to_last(k):
        return remote(
            cur.at[k, 1], cur.at[k, planes + 1], side_send.at[1], side_recv.at[1, k % 2],
            gx=at_x - 1)

    def send_layers(k):
        @pl.when(has_high)
        def _():
            to_next(k).start()

        @pl.when(has_low)
        def _():
            to_last(k).start()

    def send_planes(k, x):
        to_peer(k, x).start()

        @pl.when(jnp.logical_and(x == planes - 1, has_high))
        def _():
            to_next(k).start()

        @pl.when(jnp.logical_and(x == 0, has_low))
        def _():
            to_last(k).start()

    def send_edges(k, x, field):
        for n in range(local):
            for v in range(nvar):
                at = n * nvar + v
                edge_out[k, x, 1, at:at + 1] = field[n][v][:1]
                edge_out[k, x, 0, at:at + 1] = field[n][v][rows - 1:]

    def start_edges(k, x):
        to_side(k, x, 0).start()
        to_side(k, x, 1).start()

    def mine(k, x):
        return [[cur[k, x + 1, n, v] for v in range(nvar)] for n in range(local)]

    even = core == 0

    def weights_of(hop, a):
        own = [derivative(2 * local * hop + a - b, total) for b in range(local)]
        other = [
            jnp.where(
                even,
                jnp.float32(derivative(2 * local * hop - local + a - b, total)),
                jnp.float32(derivative(2 * local * hop + local + a - b, total)),
            )
            for b in range(local)
        ]
        return own + other

    def send_parts(k, x):
        to_peer(k, x).wait_recv()
        for hop in hops:
            for a in range(local):
                weights = weights_of(hop, a)
                for v in range(nvar):
                    pieces = [cur[k, x + 1, b, v] for b in range(local)]
                    pieces += [peer[k, x, b, v] for b in range(local)]
                    part[k - 1, hop - 1, x, a, v] = weighted(weights, pieces)
            to_pair(k, x, hop).start()

    for step in range(planes):
        load_state(plane_of(step), 0 if step == 0 else 4).start()

    barrier = pltpu.get_barrier_semaphore()

    def greet(**where):
        pl.semaphore_signal(barrier, inc=1, device_id=where, device_id_type=MESH)

    leads = core == 1
    tail = pair * 2
    counts_inst = rank == ranks - 1
    counts_side = rank == 1

    @pl.when(jnp.logical_not(counts_inst))
    def _():
        greet(inst=ranks - 1)

    greet(inst=tail, gy=up)
    greet(inst=tail, gy=down)

    @pl.when(has_low)
    def _():
        greet(inst=1, gx=at_x - 1)

    @pl.when(has_high)
    def _():
        greet(inst=1, gx=at_x + 1)

    for copy in loads:
        copy.start(priority=1)

    zero = jnp.zeros((local, nvar, rows, depth), jnp.float32)

    @pl.when(jnp.logical_not(has_low))
    def _():
        for k in range(ITERS):
            cur[k, 0] = zero

    @pl.when(jnp.logical_not(has_high))
    def _():
        for k in range(ITERS):
            cur[k, planes + 1] = zero

    sides = has_low.astype(jnp.int32) + has_high.astype(jnp.int32)
    rest = cur.at[0, 1:planes]

    def tell(stage, where):
        pl.semaphore_signal(
            ready.at[stage], inc=1, device_id={"inst": where}, device_id_type=MESH)

    def gather(stage, counts, arrivals, others):
        @pl.when(counts)
        def _():
            pl.semaphore_wait(barrier, arrivals)
            for where in others:
                tell(stage, where)

        @pl.when(jnp.logical_not(counts))
        def _():
            pl.semaphore_wait(ready.at[stage], 1)

    gather(0, counts_inst, ranks - 1, range(ranks - 1))
    load_state(plane_of(0), 0).wait()

    for hop in hops:
        to_pair(0, plane_of(0), hop).start()

    pltpu.make_async_copy(rest, rest, load_sem.at[4]).wait()

    @pl.loop(1, planes)
    def _(step):
        for hop in hops:
            to_pair(0, plane_of(step), hop).start()

    @pl.loop(0, planes)
    def _(step):
        to_peer(0, plane_of(step)).start()

    def first_layers():
        gather(1, counts_side, ranks * sides, [at for at in range(ranks) if at != 1])
        send_layers(0)

    @pl.when(at_y % 2 == 0)
    def _():
        first_layers()

    gather(2, jnp.logical_not(leads), 4, [partner])

    @pl.loop(0, planes)
    def _(step):
        x = plane_of(step)
        send_edges(0, x, mine(0, x))
        start_edges(0, x)

    @pl.when(at_y % 2 == 1)
    def _():
        first_layers()
    pltpu.make_async_copy(cells, cells, load_sem.at[1]).wait()
    for copy in loads[2:]:
        copy.wait()

    @pl.loop(0, planes)
    def _(step):
        x = plane_of(step)
        for n in range(local):
            matrix = factor([[cells[n, v, w, x] for w in range(nvar)] for v in range(nvar)])
            for v in range(nvar):
                for w in range(nvar):
                    lu[n, v, w, x] = matrix[v][w]

    row_at = lax.broadcasted_iota(jnp.int32, (rows, depth), 0)
    lane_at = lax.broadcasted_iota(jnp.int32, (rows, depth), 1)
    first_row, final_row = row_at == 0, row_at == rows - 1
    first_lane, final_lane = lane_at == 0, lane_at == depth - 1
    speed = speed_in[0]
    def lag_of(k):
        return jnp.where(jnp.logical_and(leads, k == ITERS - 1), min(5, planes), min(LAG, planes))


    def near_side(k, x):
        result = [[None] * nvar for _ in range(local)]
        for w in range(nvar):
            for n in range(local):
                field = cur[k, x + 1, n, w]
                at = n * nvar + w
                shifted = [
                    cur[k, x, n, w],
                    cur[k, x + 2, n, w],
                    jnp.where(first_row, edge_in[k, x, 0, at:at + 1], pltpu.roll(field, 1, 0)),
                    jnp.where(
                        final_row, edge_in[k, x, 1, at:at + 1], pltpu.roll(field, rows - 1, 0)),
                    jnp.where(first_lane, 0.0, pltpu.roll(field, 1, 1)),
                    jnp.where(final_lane, 0.0, pltpu.roll(field, depth - 1, 1)),
                ]
                for v in range(nvar):
                    term = weighted([weights_in[v, d, w] for d in range(6)], shifted)
                    last = result[n][v]
                    result[n][v] = term if last is None else last + term
        for n in range(local):
            weights = weights_of(0, n)
            for v in range(nvar):
                pieces = [cur[k, x + 1, b, v] for b in range(local)]
                pieces += [peer[k, x, b, v] for b in range(local)]
                spectral = weighted(weights, pieces)
                result[n][v] = cells[n, v, nvar, x] - result[n][v] - speed * spectral
        return result

    def far_side(k, x, n, v):
        spectral = None
        for hop in hops:
            if k == 0:
                pieces = [got[k, hop - 1, x, b, v] for b in range(local)]
                pieces += [peer[ITERS + hop - 1, x, b, v] for b in range(local)]
                term = weighted(weights_of(hop, n), pieces)
            else:
                term = got[k, hop - 1, x, n, v]
            spectral = term if spectral is None else spectral + term
        return spectral

    def pass_on(x):
        for hop in hops:
            to_pair(0, x, hop).wait_recv()
            relay(x, hop).start()

    pass_on(plane_of(0))
    pltpu.make_async_copy(peer.at[0], peer.at[0], first_recv.at[0]).wait()

    for k in range(ITERS):
        final_pass = k == ITERS - 1

        @pl.loop(0, planes)
        def _(step, k=k, final_pass=final_pass):
            x = plane_of(step)

            @pl.when(jnp.logical_and(x == 0, has_low))
            def _():
                to_next(k).wait_recv()

            @pl.when(jnp.logical_and(x == planes - 1, has_high))
            def _():
                to_last(k).wait_recv()

            @pl.when(step % group == 0)
            def _():
                both_sides(k, x).wait_recv()

            rights = near_side(k, x)
            if final_pass:
                own = mine(k, x)
                for n in range(local):
                    for v in range(nvar):
                        for w in range(nvar):
                            rights[n][v] = rights[n][v] - cells[n, v, w, x] * own[n][w]
            if k == 0:

                @pl.when(step + 1 < planes)
                def _():
                    pass_on(plane_of(step + 1))

                for hop in hops:
                    relay(x, hop).wait_recv()
            else:
                for hop in hops:
                    to_pair(k, x, hop).wait_recv()
            fields = []
            for n in range(local):
                right = rights[n]
                if pairs > 1:
                    right = [right[v] - speed * far_side(k, x, n, v) for v in range(nvar)]
                answer = substitute(lambda v, w: lu[n, v, w, x], right)
                for v in range(nvar):
                    if final_pass:
                        last_residual[n, v, x] = right[v]
                        state_next[n, v, x] = own[n][v] + answer[v]
                    else:
                        cur[k + 1, x + 1, n, v] = answer[v]
                fields.append(answer)
            if not final_pass:
                send_edges(k + 1, x, fields)
                send_planes(k + 1, x)
                start_edges(k + 1, x)

                later = lag_of(k + 1)

                @pl.when(step >= later)
                def _():
                    send_parts(k + 1, plane_of(step - later))

            if k > 0:
                now = lag_of(k)

                for j in range(2):
                    at = step * 2 + j

                    @pl.when(at < now)
                    def _(at=at):
                        send_parts(k, plane_of(planes - now + at))

    for hop in hops:
        sent = got.at[:, hop - 1]
        remote(sent, sent, x_send.at[0], x_send.at[0], inst=partner).wait_send()
    remote(peer, peer, core_send.at[0], core_send.at[0], inst=partner).wait_send()
    remote(edge_out, edge_out, edge_send.at[0], edge_send.at[0], inst=partner).wait_send()
    layer = cur.at[:, 0]

    @pl.when(has_high)
    def _():
        remote(layer, layer, side_send.at[0], side_send.at[0], inst=partner).wait_send()

    @pl.when(has_low)
    def _():
        remote(layer, layer, side_send.at[1], side_send.at[1], inst=partner).wait_send()


def store(field, residual, state_next, last_residual, sems):
    copies = [
        pltpu.make_async_copy(field, state_next, sems.at[0]),
        pltpu.make_async_copy(residual, last_residual, sems.at[1]),
    ]
    for queue, copy in enumerate(copies):
        copy.start(priority=queue)
    for copy in copies:
        copy.wait()


def solution(mesh):
    ranks, count_x, count_y = mesh.shape["inst"], mesh.shape["gx"], mesh.shape["gy"]

    def shards(state, source, jacobian, couplings, omega):
        local, nvar, planes, rows, depth = state.shape
        pairs = ranks // 2
        cell = (local, nvar, rows, depth)
        group = GROUP if planes % GROUP == 0 else 1
        edge = pltpu.VMEM((ITERS, planes, 2, local * nvar, depth), jnp.float32)
        hbm = pl.BlockSpec(memory_space=pltpu.HBM)
        near = pl.BlockSpec(memory_space=pltpu.VMEM)
        dma = pltpu.SemaphoreType.DMA
        vmem = lambda *lead: pltpu.VMEM(lead + cell, jnp.float32)
        matrices = pltpu.VMEM(jacobian.shape, jnp.float32)
        padded = (local, nvar, nvar + 1, planes, rows, depth)
        flows = couplings.transpose(1, 0, 2)
        field, residual = pl.pallas_call(
            functools.partial(kernel, ranks, count_x, count_y),
            out_shape=[pltpu.VMEM(state.shape, jnp.float32)] * 2,
            in_specs=[hbm] * 5,
            out_specs=[near, near],
            scratch_shapes=[
                vmem(ITERS, planes + 2), vmem(ITERS + pairs - 1, planes),
                vmem(ITERS - 1, pairs - 1, planes), vmem(ITERS, pairs - 1, planes),
                edge, edge, pltpu.VMEM(padded, jnp.float32), matrices,
                pltpu.SMEM(flows.shape, jnp.float32), pltpu.SMEM(omega.shape, jnp.float32),
                dma((5,)), dma((1,)), dma((1,)), dma((1,)), dma((2,)),
                dma((1,)), dma((3 * (pairs - 1), planes)),
                dma((2, planes // group)), dma((2, 2)),
                pltpu.SemaphoreType.REGULAR((3,)),
            ],
            compiler_params=pltpu.CompilerParams(
                collective_id=0, has_side_effects=True, vmem_limit_bytes=60 * 1024 * 1024),
            name="smooth",
        )(state, source, jacobian, flows, omega)
        return tuple(pl.pallas_call(
            store,
            out_shape=[jax.ShapeDtypeStruct(state.shape, jnp.float32)] * 2,
            in_specs=[near, near],
            out_specs=[hbm, hbm],
            scratch_shapes=[dma((2,))],
            compiler_params=pltpu.CompilerParams(vmem_limit_bytes=16 * 1024 * 1024),
            name="store",
        )(field, residual))

    split = P("inst", None, "gx", "gy", None)
    return jax.shard_map(
        shards,
        mesh=mesh,
        in_specs=(split, split, P("inst", None, None, "gx", "gy", None), P(), P()),
        out_specs=(split, split),
        check_vma=False,
    )
```

```python
import functools
import math

import jax
import jax.numpy as jnp
from jax import lax
from jax.experimental import pallas as pl
from jax.experimental.pallas import tpu as pltpu
from jax.sharding import PartitionSpec as P

ITERS = 3
LAG = 1
GROUP = 2
MESH = pl.DeviceIdType.MESH


def derivative(offset, total):
    offset = offset % total
    if offset > total // 2:
        offset -= total
    if offset == 0:
        return 0.0
    angle = math.pi * offset / total
    return 0.5 * (-1.0) ** offset * math.cos(angle) / math.sin(angle)


def factor(blocks):
    size = len(blocks)
    matrix = [list(row) for row in blocks]
    for pivot in range(size):
        matrix[pivot][pivot] = 1.0 / matrix[pivot][pivot]
        for target in range(pivot + 1, size):
            ratio = matrix[target][pivot] * matrix[pivot][pivot]
            matrix[target][pivot] = ratio
            for column in range(pivot + 1, size):
                matrix[target][column] = matrix[target][column] - ratio * matrix[pivot][column]
    return matrix


def substitute(matrix, right):
    size = len(right)
    vector = list(right)
    for pivot in range(size):
        for target in range(pivot + 1, size):
            vector[target] = vector[target] - matrix(target, pivot) * vector[pivot]
    result = [None] * size
    for pivot in reversed(range(size)):
        total = vector[pivot]
        for column in range(pivot + 1, size):
            total = total - matrix(pivot, column) * result[column]
        result[pivot] = total * matrix(pivot, pivot)
    return result


def weighted(weights, pieces):
    total = None
    for weight, piece in zip(weights, pieces):
        if isinstance(weight, float) and weight == 0.0:
            continue
        term = weight * piece
        total = term if total is None else total + term
    return total


def kernel(
    ranks, count_x, count_y,
    state, source, jacobian, couplings, omega,
    state_next, last_residual,
    cur, peer, part, got, edge_out, edge_in,
    cells, lu, weights_in, speed_in,
    load_sem, x_send, core_send, edge_send, side_send,
    first_recv, plane_recv, edge_recv, side_recv, ready,
):
    local, nvar, planes, rows, depth = state.shape
    total = local * ranks
    pairs = ranks // 2
    rank = lax.axis_index("inst")
    at_x = lax.axis_index("gx")
    at_y = lax.axis_index("gy")
    pair = rank // 2
    core = rank % 2
    partner = pair * 2 + 1 - core
    up = (at_y + 1) % count_y
    down = (at_y + count_y - 1) % count_y
    has_low = at_x > 0
    has_high = at_x < count_x - 1
    flip = at_x % 2 == 0
    hops = range(1, pairs)
    group = GROUP if planes % GROUP == 0 else 1

    def plane_of(step):
        return jnp.where(flip, planes - 1 - step, step)

    def load_state(x, at):
        return pltpu.make_async_copy(state.at[:, :, x], cur.at[0, x + 1], load_sem.at[at])

    loads = [
        pltpu.make_async_copy(jacobian, cells.at[:, :, :nvar], load_sem.at[1]),
        pltpu.make_async_copy(source, cells.at[:, :, nvar], load_sem.at[1]),
        pltpu.make_async_copy(couplings, weights_in, load_sem.at[2]),
        pltpu.make_async_copy(omega, speed_in, load_sem.at[3]),
    ]

    def remote(source_ref, target_ref, send, recv, **where):
        return pltpu.make_async_remote_copy(
            source_ref, target_ref, send, recv, device_id=where, device_id_type=MESH)

    def to_peer(k, x):
        recv = first_recv.at[0] if k == 0 else plane_recv.at[k - 1, x]
        return remote(cur.at[k, x + 1], peer.at[k, x], core_send.at[0], recv, inst=partner)

    def to_pair(k, x, hop):
        target = ((pair + hop) % pairs) * 2 + core
        outgoing = cur.at[0, x + 1] if k == 0 else part.at[k - 1, hop - 1, x]
        return remote(
            outgoing, got.at[k, hop - 1, x], x_send.at[0],
            plane_recv.at[3 * hop - 3 + 2 * (k % 2), x], inst=target)

    def relay(x, hop):
        return remote(
            got.at[0, hop - 1, x], peer.at[ITERS + hop - 1, x], core_send.at[0],
            plane_recv.at[3 * hop - 2, x], inst=partner)

    def to_side(k, x, side):
        return remote(
            edge_out.at[k, x, side], edge_in.at[k, x, side], edge_send.at[0],
            edge_recv.at[k % 2, x // group], gy=up if side == 0 else down)

    def both_sides(k, x):
        some = edge_in.at[k, :group]
        return remote(some, some, edge_send.at[0], edge_recv.at[k % 2, x // group], gy=up)

    def to_next(k):
        return remote(
            cur.at[k, planes], cur.at[k, 0], side_send.at[0], side_recv.at[0, k % 2], gx=at_x + 1)

    def to_last(k):
        return remote(
            cur.at[k, 1], cur.at[k, planes + 1], side_send.at[1], side_recv.at[1, k % 2],
            gx=at_x - 1)

    def send_layers(k):
        @pl.when(has_high)
        def _():
            to_next(k).start()

        @pl.when(has_low)
        def _():
            to_last(k).start()

    def send_planes(k, x):
        to_peer(k, x).start()

        @pl.when(jnp.logical_and(x == planes - 1, has_high))
        def _():
            to_next(k).start()

        @pl.when(jnp.logical_and(x == 0, has_low))
        def _():
            to_last(k).start()

    def send_edges(k, x, field):
        for n in range(local):
            for v in range(nvar):
                at = n * nvar + v
                edge_out[k, x, 1, at:at + 1] = field[n][v][:1]
                edge_out[k, x, 0, at:at + 1] = field[n][v][rows - 1:]

    def start_edges(k, x):
        to_side(k, x, 0).start()
        to_side(k, x, 1).start()

    def mine(k, x):
        return [[cur[k, x + 1, n, v] for v in range(nvar)] for n in range(local)]

    even = core == 0

    def weights_of(hop, a):
        own = [derivative(2 * local * hop + a - b, total) for b in range(local)]
        other = [
            jnp.where(
                even,
                jnp.float32(derivative(2 * local * hop - local + a - b, total)),
                jnp.float32(derivative(2 * local * hop + local + a - b, total)),
            )
            for b in range(local)
        ]
        return own + other

    def send_parts(k, x):
        to_peer(k, x).wait_recv()
        for hop in hops:
            for a in range(local):
                weights = weights_of(hop, a)
                for v in range(nvar):
                    pieces = [cur[k, x + 1, b, v] for b in range(local)]
                    pieces += [peer[k, x, b, v] for b in range(local)]
                    part[k - 1, hop - 1, x, a, v] = weighted(weights, pieces)
            to_pair(k, x, hop).start()

    for step in range(planes):
        load_state(plane_of(step), 0 if step == 0 else 4).start()

    barrier = pltpu.get_barrier_semaphore()

    def greet(**where):
        pl.semaphore_signal(barrier, inc=1, device_id=where, device_id_type=MESH)

    leads = core == 1
    tail = pair * 2
    counts_inst = rank == ranks - 1
    counts_side = rank == 1

    @pl.when(jnp.logical_not(counts_inst))
    def _():
        greet(inst=ranks - 1)

    greet(inst=tail, gy=up)
    greet(inst=tail, gy=down)

    @pl.when(has_low)
    def _():
        greet(inst=1, gx=at_x - 1)

    @pl.when(has_high)
    def _():
        greet(inst=1, gx=at_x + 1)

    for copy in loads:
        copy.start()

    zero = jnp.zeros((local, nvar, rows, depth), jnp.float32)

    @pl.when(jnp.logical_not(has_low))
    def _():
        for k in range(ITERS):
            cur[k, 0] = zero

    @pl.when(jnp.logical_not(has_high))
    def _():
        for k in range(ITERS):
            cur[k, planes + 1] = zero

    sides = has_low.astype(jnp.int32) + has_high.astype(jnp.int32)
    rest = cur.at[0, 1:planes]

    def tell(stage, where):
        pl.semaphore_signal(
            ready.at[stage], inc=1, device_id={"inst": where}, device_id_type=MESH)

    def gather(stage, counts, arrivals, others):
        @pl.when(counts)
        def _():
            pl.semaphore_wait(barrier, arrivals)
            for where in others:
                tell(stage, where)

        @pl.when(jnp.logical_not(counts))
        def _():
            pl.semaphore_wait(ready.at[stage], 1)

    gather(0, counts_inst, ranks - 1, range(ranks - 1))
    load_state(plane_of(0), 0).wait()

    for hop in hops:
        to_pair(0, plane_of(0), hop).start()

    pltpu.make_async_copy(rest, rest, load_sem.at[4]).wait()

    @pl.loop(1, planes)
    def _(step):
        for hop in hops:
            to_pair(0, plane_of(step), hop).start()

    @pl.loop(0, planes)
    def _(step):
        to_peer(0, plane_of(step)).start()

    def first_layers():
        gather(1, counts_side, ranks * sides, [at for at in range(ranks) if at != 1])
        send_layers(0)

    @pl.when(at_y % 2 == 0)
    def _():
        first_layers()

    gather(2, jnp.logical_not(leads), 4, [partner])

    @pl.loop(0, planes)
    def _(step):
        x = plane_of(step)
        send_edges(0, x, mine(0, x))
        start_edges(0, x)

    @pl.when(at_y % 2 == 1)
    def _():
        first_layers()
    pltpu.make_async_copy(cells, cells, load_sem.at[1]).wait()
    for copy in loads[2:]:
        copy.wait()

    @pl.loop(0, planes)
    def _(step):
        x = plane_of(step)
        for n in range(local):
            matrix = factor([[cells[n, v, w, x] for w in range(nvar)] for v in range(nvar)])
            for v in range(nvar):
                for w in range(nvar):
                    lu[n, v, w, x] = matrix[v][w]

    row_at = lax.broadcasted_iota(jnp.int32, (rows, depth), 0)
    lane_at = lax.broadcasted_iota(jnp.int32, (rows, depth), 1)
    first_row, final_row = row_at == 0, row_at == rows - 1
    first_lane, final_lane = lane_at == 0, lane_at == depth - 1
    speed = speed_in[0]
    def lag_of(k):
        return jnp.where(jnp.logical_and(leads, k == ITERS - 1), min(6, planes), min(LAG, planes))


    def near_side(k, x):
        result = [[None] * nvar for _ in range(local)]
        for w in range(nvar):
            for n in range(local):
                field = cur[k, x + 1, n, w]
                at = n * nvar + w
                shifted = [
                    cur[k, x, n, w],
                    cur[k, x + 2, n, w],
                    jnp.where(first_row, edge_in[k, x, 0, at:at + 1], pltpu.roll(field, 1, 0)),
                    jnp.where(
                        final_row, edge_in[k, x, 1, at:at + 1], pltpu.roll(field, rows - 1, 0)),
                    jnp.where(first_lane, 0.0, pltpu.roll(field, 1, 1)),
                    jnp.where(final_lane, 0.0, pltpu.roll(field, depth - 1, 1)),
                ]
                for v in range(nvar):
                    term = weighted([weights_in[v, d, w] for d in range(6)], shifted)
                    last = result[n][v]
                    result[n][v] = term if last is None else last + term
        for n in range(local):
            weights = weights_of(0, n)
            for v in range(nvar):
                pieces = [cur[k, x + 1, b, v] for b in range(local)]
                pieces += [peer[k, x, b, v] for b in range(local)]
                spectral = weighted(weights, pieces)
                result[n][v] = cells[n, v, nvar, x] - result[n][v] - speed * spectral
        return result

    def far_side(k, x, n, v):
        spectral = None
        for hop in hops:
            if k == 0:
                pieces = [got[k, hop - 1, x, b, v] for b in range(local)]
                pieces += [peer[ITERS + hop - 1, x, b, v] for b in range(local)]
                term = weighted(weights_of(hop, n), pieces)
            else:
                term = got[k, hop - 1, x, n, v]
            spectral = term if spectral is None else spectral + term
        return spectral

    def pass_on(x):
        for hop in hops:
            to_pair(0, x, hop).wait_recv()
            relay(x, hop).start()

    pass_on(plane_of(0))
    pltpu.make_async_copy(peer.at[0], peer.at[0], first_recv.at[0]).wait()

    for k in range(ITERS):
        final_pass = k == ITERS - 1

        @pl.loop(0, planes)
        def _(step, k=k, final_pass=final_pass):
            x = plane_of(step)

            @pl.when(jnp.logical_and(x == 0, has_low))
            def _():
                to_next(k).wait_recv()

            @pl.when(jnp.logical_and(x == planes - 1, has_high))
            def _():
                to_last(k).wait_recv()

            @pl.when(step % group == 0)
            def _():
                both_sides(k, x).wait_recv()

            rights = near_side(k, x)
            if final_pass:
                own = mine(k, x)
                for n in range(local):
                    for v in range(nvar):
                        for w in range(nvar):
                            rights[n][v] = rights[n][v] - cells[n, v, w, x] * own[n][w]
            if k == 0:

                @pl.when(step + 1 < planes)
                def _():
                    pass_on(plane_of(step + 1))

                for hop in hops:
                    relay(x, hop).wait_recv()
            else:
                for hop in hops:
                    to_pair(k, x, hop).wait_recv()
            fields = []
            for n in range(local):
                right = rights[n]
                if pairs > 1:
                    right = [right[v] - speed * far_side(k, x, n, v) for v in range(nvar)]
                answer = substitute(lambda v, w: lu[n, v, w, x], right)
                for v in range(nvar):
                    if final_pass:
                        last_residual[n, v, x] = right[v]
                        state_next[n, v, x] = own[n][v] + answer[v]
                    else:
                        cur[k + 1, x + 1, n, v] = answer[v]
                fields.append(answer)
            if not final_pass:
                send_edges(k + 1, x, fields)
                send_planes(k + 1, x)
                start_edges(k + 1, x)

                later = lag_of(k + 1)

                @pl.when(step >= later)
                def _():
                    send_parts(k + 1, plane_of(step - later))

            if k > 0:
                now = lag_of(k)

                for j in range(6):
                    at = step * 6 + j

                    @pl.when(at < now)
                    def _(at=at):
                        send_parts(k, plane_of(planes - now + at))

    for hop in hops:
        sent = got.at[:, hop - 1]
        remote(sent, sent, x_send.at[0], x_send.at[0], inst=partner).wait_send()
    remote(peer, peer, core_send.at[0], core_send.at[0], inst=partner).wait_send()
    remote(edge_out, edge_out, edge_send.at[0], edge_send.at[0], inst=partner).wait_send()
    layer = cur.at[:, 0]

    @pl.when(has_high)
    def _():
        remote(layer, layer, side_send.at[0], side_send.at[0], inst=partner).wait_send()

    @pl.when(has_low)
    def _():
        remote(layer, layer, side_send.at[1], side_send.at[1], inst=partner).wait_send()


def store(field, residual, state_next, last_residual, sems):
    copies = [
        pltpu.make_async_copy(field, state_next, sems.at[0]),
        pltpu.make_async_copy(residual, last_residual, sems.at[1]),
    ]
    for copy in copies:
        copy.start()
    for copy in copies:
        copy.wait()


def solution(mesh):
    ranks, count_x, count_y = mesh.shape["inst"], mesh.shape["gx"], mesh.shape["gy"]

    def shards(state, source, jacobian, couplings, omega):
        local, nvar, planes, rows, depth = state.shape
        pairs = ranks // 2
        cell = (local, nvar, rows, depth)
        group = GROUP if planes % GROUP == 0 else 1
        edge = pltpu.VMEM((ITERS, planes, 2, local * nvar, depth), jnp.float32)
        hbm = pl.BlockSpec(memory_space=pltpu.HBM)
        near = pl.BlockSpec(memory_space=pltpu.VMEM)
        dma = pltpu.SemaphoreType.DMA
        vmem = lambda *lead: pltpu.VMEM(lead + cell, jnp.float32)
        matrices = pltpu.VMEM(jacobian.shape, jnp.float32)
        padded = (local, nvar, nvar + 1, planes, rows, depth)
        flows = couplings.transpose(1, 0, 2)
        field, residual = pl.pallas_call(
            functools.partial(kernel, ranks, count_x, count_y),
            out_shape=[pltpu.VMEM(state.shape, jnp.float32)] * 2,
            in_specs=[hbm] * 5,
            out_specs=[near, near],
            scratch_shapes=[
                vmem(ITERS, planes + 2), vmem(ITERS + pairs - 1, planes),
                vmem(ITERS - 1, pairs - 1, planes), vmem(ITERS, pairs - 1, planes),
                edge, edge, pltpu.VMEM(padded, jnp.float32), matrices,
                pltpu.SMEM(flows.shape, jnp.float32), pltpu.SMEM(omega.shape, jnp.float32),
                dma((5,)), dma((1,)), dma((1,)), dma((1,)), dma((2,)),
                dma((1,)), dma((3 * (pairs - 1), planes)),
                dma((2, planes // group)), dma((2, 2)),
                pltpu.SemaphoreType.REGULAR((3,)),
            ],
            compiler_params=pltpu.CompilerParams(
                collective_id=0, has_side_effects=True, vmem_limit_bytes=60 * 1024 * 1024),
            name="smooth",
        )(state, source, jacobian, flows, omega)
        return tuple(pl.pallas_call(
            store,
            out_shape=[jax.ShapeDtypeStruct(state.shape, jnp.float32)] * 2,
            in_specs=[near, near],
            out_specs=[hbm, hbm],
            scratch_shapes=[dma((2,))],
            compiler_params=pltpu.CompilerParams(vmem_limit_bytes=16 * 1024 * 1024),
            name="store",
        )(field, residual))

    split = P("inst", None, "gx", "gy", None)
    return jax.shard_map(
        shards,
        mesh=mesh,
        in_specs=(split, split, P("inst", None, None, "gx", "gy", None), P(), P()),
        out_specs=(split, split),
        check_vma=False,
    )
```

```python
import functools
import math

import jax
import jax.numpy as jnp
from jax import lax
from jax.experimental import pallas as pl
from jax.experimental.pallas import tpu as pltpu
from jax.sharding import PartitionSpec as P

ITERS = 3
LAG = 1
GROUP = 2
MESH = pl.DeviceIdType.MESH


def derivative(offset, total):
    offset = offset % total
    if offset > total // 2:
        offset -= total
    if offset == 0:
        return 0.0
    angle = math.pi * offset / total
    return 0.5 * (-1.0) ** offset * math.cos(angle) / math.sin(angle)


def factor(blocks):
    size = len(blocks)
    matrix = [list(row) for row in blocks]
    for pivot in range(size):
        matrix[pivot][pivot] = 1.0 / matrix[pivot][pivot]
        for target in range(pivot + 1, size):
            ratio = matrix[target][pivot] * matrix[pivot][pivot]
            matrix[target][pivot] = ratio
            for column in range(pivot + 1, size):
                matrix[target][column] = matrix[target][column] - ratio * matrix[pivot][column]
    return matrix


def substitute(matrix, right):
    size = len(right)
    vector = list(right)
    for pivot in range(size):
        for target in range(pivot + 1, size):
            vector[target] = vector[target] - matrix(target, pivot) * vector[pivot]
    result = [None] * size
    for pivot in reversed(range(size)):
        total = vector[pivot]
        for column in range(pivot + 1, size):
            total = total - matrix(pivot, column) * result[column]
        result[pivot] = total * matrix(pivot, pivot)
    return result


def weighted(weights, pieces):
    total = None
    for weight, piece in zip(weights, pieces):
        if isinstance(weight, float) and weight == 0.0:
            continue
        term = weight * piece
        total = term if total is None else total + term
    return total


def kernel(
    ranks, count_x, count_y,
    state, source, jacobian, couplings, omega,
    state_next, last_residual,
    cur, peer, part, got, edge_out, edge_in,
    cells, lu, weights_in, speed_in,
    load_sem, x_send, core_send, edge_send, side_send,
    first_recv, plane_recv, edge_recv, side_recv, ready,
):
    local, nvar, planes, rows, depth = state.shape
    total = local * ranks
    pairs = ranks // 2
    rank = lax.axis_index("inst")
    at_x = lax.axis_index("gx")
    at_y = lax.axis_index("gy")
    pair = rank // 2
    core = rank % 2
    partner = pair * 2 + 1 - core
    up = (at_y + 1) % count_y
    down = (at_y + count_y - 1) % count_y
    has_low = at_x > 0
    has_high = at_x < count_x - 1
    flip = at_x % 2 == 0
    hops = range(1, pairs)
    group = GROUP if planes % GROUP == 0 else 1

    def plane_of(step):
        return jnp.where(flip, planes - 1 - step, step)

    def load_state(x, at):
        return pltpu.make_async_copy(state.at[:, :, x], cur.at[0, x + 1], load_sem.at[at])

    loads = [
        pltpu.make_async_copy(jacobian, cells.at[:, :, :nvar], load_sem.at[1]),
        pltpu.make_async_copy(source, cells.at[:, :, nvar], load_sem.at[1]),
        pltpu.make_async_copy(couplings, weights_in, load_sem.at[2]),
        pltpu.make_async_copy(omega, speed_in, load_sem.at[3]),
    ]

    def remote(source_ref, target_ref, send, recv, **where):
        return pltpu.make_async_remote_copy(
            source_ref, target_ref, send, recv, device_id=where, device_id_type=MESH)

    def to_peer(k, x):
        recv = first_recv.at[0] if k == 0 else plane_recv.at[k - 1, x]
        return remote(cur.at[k, x + 1], peer.at[k, x], core_send.at[0], recv, inst=partner)

    def to_pair(k, x, hop):
        target = ((pair + hop) % pairs) * 2 + core
        outgoing = cur.at[0, x + 1] if k == 0 else part.at[k - 1, hop - 1, x]
        return remote(
            outgoing, got.at[k, hop - 1, x], x_send.at[0],
            plane_recv.at[3 * hop - 3 + 2 * (k % 2), x], inst=target)

    def relay(x, hop):
        return remote(
            got.at[0, hop - 1, x], peer.at[ITERS + hop - 1, x], core_send.at[0],
            plane_recv.at[3 * hop - 2, x], inst=partner)

    def to_side(k, x, side):
        return remote(
            edge_out.at[k, x, side], edge_in.at[k, x, side], edge_send.at[0],
            edge_recv.at[k % 2, x // group], gy=up if side == 0 else down)

    def both_sides(k, x):
        some = edge_in.at[k, :group]
        return remote(some, some, edge_send.at[0], edge_recv.at[k % 2, x // group], gy=up)

    def to_next(k):
        return remote(
            cur.at[k, planes], cur.at[k, 0], side_send.at[0], side_recv.at[0, k % 2], gx=at_x + 1)

    def to_last(k):
        return remote(
            cur.at[k, 1], cur.at[k, planes + 1], side_send.at[1], side_recv.at[1, k % 2],
            gx=at_x - 1)

    def send_layers(k):
        @pl.when(has_high)
        def _():
            to_next(k).start()

        @pl.when(has_low)
        def _():
            to_last(k).start()

    def send_planes(k, x):
        to_peer(k, x).start()

        @pl.when(jnp.logical_and(x == planes - 1, has_high))
        def _():
            to_next(k).start()

        @pl.when(jnp.logical_and(x == 0, has_low))
        def _():
            to_last(k).start()

    def send_edges(k, x, field):
        for n in range(local):
            for v in range(nvar):
                at = n * nvar + v
                edge_out[k, x, 1, at:at + 1] = field[n][v][:1]
                edge_out[k, x, 0, at:at + 1] = field[n][v][rows - 1:]

    def start_edges(k, x):
        to_side(k, x, 0).start()
        to_side(k, x, 1).start()

    def mine(k, x):
        return [[cur[k, x + 1, n, v] for v in range(nvar)] for n in range(local)]

    even = core == 0

    def weights_of(hop, a):
        own = [derivative(2 * local * hop + a - b, total) for b in range(local)]
        other = [
            jnp.where(
                even,
                jnp.float32(derivative(2 * local * hop - local + a - b, total)),
                jnp.float32(derivative(2 * local * hop + local + a - b, total)),
            )
            for b in range(local)
        ]
        return own + other

    def send_parts(k, x):
        to_peer(k, x).wait_recv()
        for hop in hops:
            for a in range(local):
                weights = weights_of(hop, a)
                for v in range(nvar):
                    pieces = [cur[k, x + 1, b, v] for b in range(local)]
                    pieces += [peer[k, x, b, v] for b in range(local)]
                    part[k - 1, hop - 1, x, a, v] = weighted(weights, pieces)
            to_pair(k, x, hop).start()

    barrier = pltpu.get_barrier_semaphore()

    def greet(**where):
        pl.semaphore_signal(barrier, inc=1, device_id=where, device_id_type=MESH)

    leads = core == 1
    tail = pair * 2
    counts_inst = rank == ranks - 1
    counts_side = rank == 1

    @pl.when(jnp.logical_not(counts_inst))
    def _():
        greet(inst=ranks - 1)

    for step in range(planes):
        load_state(plane_of(step), 0 if step == 0 else 4).start()

    greet(inst=tail, gy=up)
    greet(inst=tail, gy=down)

    @pl.when(has_low)
    def _():
        greet(inst=1, gx=at_x - 1)

    @pl.when(has_high)
    def _():
        greet(inst=1, gx=at_x + 1)

    sides = has_low.astype(jnp.int32) + has_high.astype(jnp.int32)
    rest = cur.at[0, 1:planes]

    def tell(stage, where):
        pl.semaphore_signal(
            ready.at[stage], inc=1, device_id={"inst": where}, device_id_type=MESH)

    def gather(stage, counts, arrivals, others):
        @pl.when(counts)
        def _():
            pl.semaphore_wait(barrier, arrivals)
            for where in others:
                tell(stage, where)

        @pl.when(jnp.logical_not(counts))
        def _():
            pl.semaphore_wait(ready.at[stage], 1)

    gather(0, counts_inst, ranks - 1, range(ranks - 2, -1, -1))
    load_state(plane_of(0), 0).wait()

    for hop in hops:
        to_pair(0, plane_of(0), hop).start()

    pltpu.make_async_copy(rest, rest, load_sem.at[4]).wait()

    @pl.loop(1, planes)
    def _(step):
        for hop in hops:
            to_pair(0, plane_of(step), hop).start()

    for copy in loads:
        copy.start(priority=1)

    @pl.loop(0, planes)
    def _(step):
        to_peer(0, plane_of(step)).start()

    zero = jnp.zeros((local, nvar, rows, depth), jnp.float32)

    @pl.when(jnp.logical_not(has_low))
    def _():
        for k in range(ITERS):
            cur[k, 0] = zero

    @pl.when(jnp.logical_not(has_high))
    def _():
        for k in range(ITERS):
            cur[k, planes + 1] = zero

    def first_layers():
        gather(1, counts_side, ranks * sides, [at for at in range(ranks) if at != 1])
        send_layers(0)

    @pl.when(at_y % 2 == 0)
    def _():
        first_layers()

    gather(2, jnp.logical_not(leads), 4, [partner])

    @pl.loop(0, planes)
    def _(step):
        x = plane_of(step)
        send_edges(0, x, mine(0, x))
        start_edges(0, x)

    @pl.when(at_y % 2 == 1)
    def _():
        first_layers()
    pltpu.make_async_copy(cells, cells, load_sem.at[1]).wait()
    for copy in loads[2:]:
        copy.wait()

    @pl.loop(0, planes)
    def _(step):
        x = plane_of(step)
        for n in range(local):
            matrix = factor([[cells[n, v, w, x] for w in range(nvar)] for v in range(nvar)])
            for v in range(nvar):
                for w in range(nvar):
                    lu[n, v, w, x] = matrix[v][w]

    row_at = lax.broadcasted_iota(jnp.int32, (rows, depth), 0)
    lane_at = lax.broadcasted_iota(jnp.int32, (rows, depth), 1)
    first_row, final_row = row_at == 0, row_at == rows - 1
    first_lane, final_lane = lane_at == 0, lane_at == depth - 1
    speed = speed_in[0]
    def lag_of(k):
        return jnp.where(jnp.logical_and(leads, k == ITERS - 1), min(5, planes), min(LAG, planes))


    def near_side(k, x):
        result = [[None] * nvar for _ in range(local)]
        for w in range(nvar):
            for n in range(local):
                field = cur[k, x + 1, n, w]
                at = n * nvar + w
                shifted = [
                    cur[k, x, n, w],
                    cur[k, x + 2, n, w],
                    jnp.where(first_row, edge_in[k, x, 0, at:at + 1], pltpu.roll(field, 1, 0)),
                    jnp.where(
                        final_row, edge_in[k, x, 1, at:at + 1], pltpu.roll(field, rows - 1, 0)),
                    jnp.where(first_lane, 0.0, pltpu.roll(field, 1, 1)),
                    jnp.where(final_lane, 0.0, pltpu.roll(field, depth - 1, 1)),
                ]
                for v in range(nvar):
                    term = weighted([weights_in[v, d, w] for d in range(6)], shifted)
                    last = result[n][v]
                    result[n][v] = term if last is None else last + term
        for n in range(local):
            weights = weights_of(0, n)
            for v in range(nvar):
                pieces = [cur[k, x + 1, b, v] for b in range(local)]
                pieces += [peer[k, x, b, v] for b in range(local)]
                spectral = weighted(weights, pieces)
                result[n][v] = cells[n, v, nvar, x] - result[n][v] - speed * spectral
        return result

    def far_side(k, x, n, v):
        spectral = None
        for hop in hops:
            if k == 0:
                pieces = [got[k, hop - 1, x, b, v] for b in range(local)]
                pieces += [peer[ITERS + hop - 1, x, b, v] for b in range(local)]
                term = weighted(weights_of(hop, n), pieces)
            else:
                term = got[k, hop - 1, x, n, v]
            spectral = term if spectral is None else spectral + term
        return spectral

    def pass_on(x):
        for hop in hops:
            to_pair(0, x, hop).wait_recv()
            relay(x, hop).start()

    pass_on(plane_of(0))
    pltpu.make_async_copy(peer.at[0], peer.at[0], first_recv.at[0]).wait()

    for k in range(ITERS):
        final_pass = k == ITERS - 1

        @pl.loop(0, planes)
        def _(step, k=k, final_pass=final_pass):
            x = plane_of(step)

            @pl.when(jnp.logical_and(x == 0, has_low))
            def _():
                to_next(k).wait_recv()

            @pl.when(jnp.logical_and(x == planes - 1, has_high))
            def _():
                to_last(k).wait_recv()

            @pl.when(step % group == 0)
            def _():
                both_sides(k, x).wait_recv()

            rights = near_side(k, x)
            if final_pass:
                own = mine(k, x)
                for n in range(local):
                    for v in range(nvar):
                        for w in range(nvar):
                            rights[n][v] = rights[n][v] - cells[n, v, w, x] * own[n][w]
            if k == 0:

                @pl.when(step + 1 < planes)
                def _():
                    pass_on(plane_of(step + 1))

                for hop in hops:
                    relay(x, hop).wait_recv()
            else:
                for hop in hops:
                    to_pair(k, x, hop).wait_recv()
            fields = []
            for n in range(local):
                right = rights[n]
                if pairs > 1:
                    right = [right[v] - speed * far_side(k, x, n, v) for v in range(nvar)]
                answer = substitute(lambda v, w: lu[n, v, w, x], right)
                for v in range(nvar):
                    if final_pass:
                        last_residual[n, v, x] = right[v]
                        state_next[n, v, x] = own[n][v] + answer[v]
                    else:
                        cur[k + 1, x + 1, n, v] = answer[v]
                fields.append(answer)
            if not final_pass:
                send_edges(k + 1, x, fields)
                send_planes(k + 1, x)
                start_edges(k + 1, x)

                later = lag_of(k + 1)

                @pl.when(step >= later)
                def _():
                    send_parts(k + 1, plane_of(step - later))

            if k > 0:
                now = lag_of(k)

                for j in range(2):
                    at = step * 2 + j

                    @pl.when(at < now)
                    def _(at=at):
                        send_parts(k, plane_of(planes - now + at))

    for hop in hops:
        sent = got.at[:, hop - 1]
        remote(sent, sent, x_send.at[0], x_send.at[0], inst=partner).wait_send()
    remote(peer, peer, core_send.at[0], core_send.at[0], inst=partner).wait_send()
    remote(edge_out, edge_out, edge_send.at[0], edge_send.at[0], inst=partner).wait_send()
    layer = cur.at[:, 0]

    @pl.when(has_high)
    def _():
        remote(layer, layer, side_send.at[0], side_send.at[0], inst=partner).wait_send()

    @pl.when(has_low)
    def _():
        remote(layer, layer, side_send.at[1], side_send.at[1], inst=partner).wait_send()


def store(field, residual, state_next, last_residual, sems):
    copies = [
        pltpu.make_async_copy(field, state_next, sems.at[0]),
        pltpu.make_async_copy(residual, last_residual, sems.at[1]),
    ]
    for copy in copies:
        copy.start()
    for copy in copies:
        copy.wait()


def solution(mesh):
    ranks, count_x, count_y = mesh.shape["inst"], mesh.shape["gx"], mesh.shape["gy"]

    def shards(state, source, jacobian, couplings, omega):
        local, nvar, planes, rows, depth = state.shape
        pairs = ranks // 2
        cell = (local, nvar, rows, depth)
        group = GROUP if planes % GROUP == 0 else 1
        edge = pltpu.VMEM((ITERS, planes, 2, local * nvar, depth), jnp.float32)
        hbm = pl.BlockSpec(memory_space=pltpu.HBM)
        near = pl.BlockSpec(memory_space=pltpu.VMEM)
        dma = pltpu.SemaphoreType.DMA
        vmem = lambda *lead: pltpu.VMEM(lead + cell, jnp.float32)
        matrices = pltpu.VMEM(jacobian.shape, jnp.float32)
        padded = (local, nvar, nvar + 1, planes, rows, depth)
        flows = couplings.transpose(1, 0, 2)
        field, residual = pl.pallas_call(
            functools.partial(kernel, ranks, count_x, count_y),
            out_shape=[pltpu.VMEM(state.shape, jnp.float32)] * 2,
            in_specs=[hbm] * 5,
            out_specs=[near, near],
            scratch_shapes=[
                vmem(ITERS, planes + 2), vmem(ITERS + pairs - 1, planes),
                vmem(ITERS - 1, pairs - 1, planes), vmem(ITERS, pairs - 1, planes),
                edge, edge, pltpu.VMEM(padded, jnp.float32), matrices,
                pltpu.SMEM(flows.shape, jnp.float32), pltpu.SMEM(omega.shape, jnp.float32),
                dma((5,)), dma((1,)), dma((1,)), dma((1,)), dma((2,)),
                dma((1,)), dma((3 * (pairs - 1), planes)),
                dma((2, planes // group)), dma((2, 2)),
                pltpu.SemaphoreType.REGULAR((3,)),
            ],
            compiler_params=pltpu.CompilerParams(
                collective_id=0, has_side_effects=True, vmem_limit_bytes=60 * 1024 * 1024),
            name="smooth",
        )(state, source, jacobian, flows, omega)
        return tuple(pl.pallas_call(
            store,
            out_shape=[jax.ShapeDtypeStruct(state.shape, jnp.float32)] * 2,
            in_specs=[near, near],
            out_specs=[hbm, hbm],
            scratch_shapes=[dma((2,))],
            compiler_params=pltpu.CompilerParams(vmem_limit_bytes=16 * 1024 * 1024),
            name="store",
        )(field, residual))

    split = P("inst", None, "gx", "gy", None)
    return jax.shard_map(
        shards,
        mesh=mesh,
        in_specs=(split, split, P("inst", None, None, "gx", "gy", None), P(), P()),
        out_specs=(split, split),
        check_vma=False,
    )
```
